32 devices in a mesh: row: 8 (over y, x, core), col: 4 (over z).
Axes of the slice: x: 2, y: 2, z: 4, core: 2. Of those that a mesh axis runs over, the one named last changes fastest.
Arguments:
- ancestor: float32 [9, 9, 512, 512], P(None, None, 'row', 'col'), may hold values from -1 to 4, as said below
- inverse_first: float32 [2, 2, 512, 512], P(None, None, 'row', 'col'), may hold values from -1 to 2, as said below
- panel_first: float32 [1536, 2, 512], P('row', None, 'col'), may hold values from -0.15625 to 0.15625
- structure_first: int32 [1536], replicated, may hold values from 0 to 4607, as said below
- inverse_second: float32 [1, 1, 512, 512], P(None, None, 'row', 'col'), may hold values from -1 to 2, as said below
- panel_second: float32 [1536, 1, 512], P('row', None, 'col'), may hold values from -0.15625 to 0.15625
- structure_second: int32 [1536], replicated, may hold values from 0 to 5631, as said below
Outputs:
- row_first: float32 [2, 11, 512, 512], P(None, None, 'row', 'col')
- row_second: float32 [1, 12, 512, 512], P(None, None, 'row', 'col')
The draws below stay inside these ranges and needn't reach their ends.
Inputs may be any that keep to these rules, and one draw needn't show every extreme that they name: `ancestor`: symmetric and positive definite as a matrix. `inverse_first`: symmetric and positive definite as a matrix. `inverse_second`: symmetric and positive definite as a matrix. `structure_first`: entries are distinct; every aligned group of 16 ancestor rows holds at most 6 entries, and some group holds exactly 6. `structure_second`: entries are distinct; every aligned group of 16 ancestor rows holds at most 6 entries, and some group holds exactly 6.
All inputs are finite; a program needn't handle non-finite values.
Results may differ from the reference program's by a relative error of at most 0.000075.
Values sent between devices are 32-bit elements; how exact they have to be, the bound alone decides.
A program may use at most 128 MiB of HBM per device.

```python
import jax
import jax.numpy as jnp
from jax import lax

ANC = 4608
WA = 1024
WB = 512
NSA = 1536
NSB = 1536
TILE = 512
GRAIN = 16
CAP = 6
RH = 64
CW = 128


def pack_tiles(tiled):
    first, second = (tiled.shape[0], tiled.shape[1])
    grid_rows = TILE // RH
    grid_cols = TILE // CW
    depth = RH * CW // 128
    blocks = tiled.reshape(first, second, grid_rows, RH, grid_cols, CW).transpose(0, 1, 2, 4, 3, 5)
    blocks = blocks.reshape(first, second, grid_rows, grid_cols, depth, 128).transpose(0, 1, 2, 4, 3, 5)
    return blocks.reshape(first, second, grid_rows * depth, grid_cols * 128)


def definite_tiles(key, row_count, floor_level, ceiling_level, spread):
    first, second = jax.random.split(key)
    noise_field = jax.random.normal(first, (row_count, row_count), jnp.float32)
    levels = jax.random.uniform(second, (row_count,), jnp.float32, floor_level, ceiling_level)
    symmetric = (noise_field + noise_field.T) * (spread / jnp.sqrt(2.0 * row_count))
    matrix = symmetric + jnp.diag(levels)
    tile_count = row_count // TILE
    return pack_tiles(matrix.reshape(tile_count, TILE, tile_count, TILE).transpose(0, 2, 1, 3))


def grouped_structure(key, row_count, entry_count):
    group_count = row_count // GRAIN
    slot_count = group_count * CAP
    first_key, second_key, third_key = jax.random.split(key, 3)
    shuffled = jax.random.permutation(first_key, slot_count).astype(jnp.int32)
    forced = jax.random.randint(second_key, (), 0, group_count).astype(jnp.int32)
    slot_group = jnp.arange(slot_count, dtype=jnp.int32) // CAP
    ranking = jnp.where(slot_group == forced, shuffled - slot_count, shuffled)
    chosen = jnp.argsort(ranking, stable=True)[:entry_count].astype(jnp.int32)
    group_keys = jax.random.split(third_key, group_count)
    offsets = jax.vmap(lambda single: jax.random.permutation(single, GRAIN)[:CAP].astype(jnp.int32))(group_keys)
    group_of = chosen // CAP
    row_ids = group_of * GRAIN + offsets[group_of, chosen % CAP]
    return row_ids.astype(jnp.int32)


def draw_ancestor(key, part):
    return definite_tiles(jax.random.fold_in(key, 11), ANC, 1.5, 3.0, 0.7)


def draw_inverse_first(key, part):
    return definite_tiles(jax.random.fold_in(key, 12), WA, 0.8, 1.5, 0.3)


def draw_inverse_second(key, part):
    return definite_tiles(jax.random.fold_in(key, 13), WB, 0.8, 1.5, 0.3)


def draw_structure_first(key, part):
    return grouped_structure(jax.random.fold_in(key, 21), ANC, NSA)


def draw_structure_second(key, part):
    return grouped_structure(jax.random.fold_in(key, 22), ANC + WA, NSB)


def shard_levels(own_key, shape, cuts, low, high):
    level = 1.0
    for dim, parts in cuts:
        steps = jax.random.uniform(jax.random.fold_in(jax.random.fold_in(own_key, 6), dim), (parts,), jnp.float32, low / len(cuts), high / len(cuts))
        level = level * jnp.repeat(jnp.exp(steps), shape[dim] // parts).reshape((-1,) + (1,) * (len(shape) - 1 - dim))
    return level


def gaussian(rng, dims, scale, limit, shards=(), held_as=jnp.bfloat16):
    array = scale * jax.random.normal(rng, dims, jnp.float32)
    if shards:
        array = array * shard_levels(rng, dims, shards, -0.22, 0.18)
    return jnp.clip(array, -limit, limit).astype(held_as)


def setup_inputs(seed: int = 0) -> dict:
    arg_keys = jax.random.split(jax.random.key(seed), 8)
    return {
        "ancestor": draw_ancestor(jax.random.fold_in(arg_keys[7], 71), 0),
        "inverse_first": draw_inverse_first(jax.random.fold_in(arg_keys[7], 71), 0),
        "panel_first": gaussian(arg_keys[2], (NSA, WA // TILE, TILE), NSA ** -0.5, 0.15625, ((0, 8), (2, 4)), jnp.float32),
        "structure_first": draw_structure_first(jax.random.fold_in(arg_keys[7], 71), 0),
        "inverse_second": draw_inverse_second(jax.random.fold_in(arg_keys[7], 71), 0),
        "panel_second": gaussian(arg_keys[5], (NSB, WB // TILE, TILE), NSB ** -0.5, 0.15625, ((0, 8), (2, 4)), jnp.float32),
        "structure_second": draw_structure_second(jax.random.fold_in(arg_keys[7], 71), 0),
    }


def unpack(packed):
    first, second = packed.shape[0], packed.shape[1]
    grid_rows = TILE // RH
    grid_cols = TILE // CW
    depth = RH * CW // 128
    blocks = packed.reshape(first, second, grid_rows, depth, grid_cols, 128).transpose(0, 1, 2, 4, 3, 5)
    blocks = blocks.reshape(first, second, grid_rows, grid_cols, RH, CW).transpose(0, 1, 2, 4, 3, 5)
    return blocks.reshape(first, second, TILE, TILE)


def pack(tiled):
    first, second = tiled.shape[0], tiled.shape[1]
    grid_rows = TILE // RH
    grid_cols = TILE // CW
    depth = RH * CW // 128
    blocks = tiled.reshape(first, second, grid_rows, RH, grid_cols, CW).transpose(0, 1, 2, 4, 3, 5)
    blocks = blocks.reshape(first, second, grid_rows, grid_cols, depth, 128).transpose(0, 1, 2, 4, 3, 5)
    return blocks.reshape(first, second, grid_rows * depth, grid_cols * 128)


def from_tiles(packed):
    tiled = unpack(packed)
    first, second, height, width = tiled.shape
    return tiled.transpose(0, 2, 1, 3).reshape(first * height, second * width)


def to_tiles(matrix):
    first = matrix.shape[0] // TILE
    second = matrix.shape[1] // TILE
    return pack(matrix.reshape(first, TILE, second, TILE).transpose(0, 2, 1, 3))


def sweep_step(frontier, inverse, panel_part, structure):
    flattened = panel_part.reshape(panel_part.shape[0], -1)
    spread = jnp.zeros((frontier.shape[0], flattened.shape[1]), jnp.float32).at[structure].set(flattened)
    image = jnp.dot(frontier, spread, precision=lax.Precision.HIGHEST, preferred_element_type=jnp.float32)
    diagonal = from_tiles(inverse) + jnp.dot(spread.T, image, precision=lax.Precision.HIGHEST, preferred_element_type=jnp.float32)
    row_block = jnp.concatenate([-image.T, diagonal], axis=1)
    upper_rows = jnp.concatenate([frontier, -image], axis=1)
    grown = jnp.concatenate([upper_rows, row_block], axis=0)
    return row_block, grown


def reference(ancestor, inverse_first, panel_first, structure_first, inverse_second, panel_second, structure_second):
    first_block, frontier = sweep_step(from_tiles(ancestor), inverse_first, panel_first, structure_first)
    second_block, unused = sweep_step(frontier, inverse_second, panel_second, structure_second)
    return to_tiles(first_block), to_tiles(second_block)
```

```python
import functools

import jax
import jax.numpy as jnp
from jax import lax
from jax.experimental import pallas as pl
from jax.experimental.pallas import tpu as pltpu
from jax.sharding import PartitionSpec as P

TILE = 512
GRAIN = 16
CAP = 6


def open_packed(packed, row_height, col_width):
    return packed.reshape(packed.shape[0], packed.shape[1], row_height, col_width)


def close_packed(tiles):
    depth = tiles.shape[2] * tiles.shape[3] // 128
    return tiles.reshape(tiles.shape[0], tiles.shape[1], depth, 128)


def product(left, right, left_dim=1):
    return lax.dot_general(
        left,
        right,
        (((left_dim,), (0,)), ((), ())),
        precision=lax.Precision.HIGH,
        preferred_element_type=jnp.float32,
    )


def entry_ranks(structure):
    group = structure // GRAIN
    order = jnp.arange(structure.shape[0], dtype=jnp.int32)
    same = (group[:, None] == group[None, :]) & (order[None, :] < order[:, None])
    return jnp.sum(same.astype(jnp.int32), axis=1)


def slots_within(structure, ranks, height):
    owner = structure % TILE // height
    group = structure // TILE * (height // GRAIN) + structure % height // GRAIN
    return owner, group * CAP + ranks


def one_hot(marks, count):
    return (jnp.arange(count, dtype=jnp.int32)[:, None] == marks[None, :]).astype(jnp.float32)


def local_rows(structure, marks, count, height):
    row = structure // TILE * height + structure % height
    match = jnp.arange(count, dtype=jnp.int32)[:, None] == marks[None, :]
    return jnp.max(jnp.where(match, row[None, :], -1), axis=1)


def on_device(
    ancestor,
    inverse_first,
    panel_first,
    structure_first,
    inverse_second,
    panel_second,
    structure_second,
):
    rows = lax.axis_size("row")
    cols = lax.axis_size("col")
    height = TILE // rows
    width = TILE // cols
    halves = width // height
    row_index = lax.axis_index("row")
    col_index = lax.axis_index("col")
    blocks = open_packed(ancestor, height, width)
    first_diag = open_packed(inverse_first, height, width)
    second_diag = open_packed(inverse_second, height, width)
    tiles = blocks.shape[0]
    first = first_diag.shape[0]
    second = second_diag.shape[0]
    every = first + second
    limit = tiles * TILE
    first_width = first * width

    panels = jnp.concatenate(
        [panel_first.reshape(-1, first_width), panel_second.reshape(-1, second * width)], axis=1
    )
    both = lax.all_gather(panels, "row", axis=0, tiled=True)
    whole_first = both[:, :first_width]
    whole_second = both[:, first_width:]

    above = structure_second < limit
    ranks_first = entry_ranks(structure_first)
    ranks_second = entry_ranks(structure_second)
    row_slots = tiles * height // GRAIN * CAP
    col_slots = tiles * width // GRAIN * CAP
    low_slots = first * TILE // GRAIN * CAP
    owner, slot = slots_within(structure_first, ranks_first, height)
    row_marks_first = jnp.where(owner == row_index, slot, -1)
    owner, slot = slots_within(structure_second, ranks_second, height)
    row_marks_second = jnp.where(above & (owner == row_index), slot, -1)
    owner, slot = slots_within(structure_first, ranks_first, width)
    all_marks_first = owner * col_slots + slot
    col_marks_first = jnp.where(owner == col_index, slot, -1)
    owner, slot = slots_within(structure_second, ranks_second, width)
    all_marks_second = jnp.where(above, owner * col_slots + slot, -1)
    col_marks_second = jnp.where(above & (owner == col_index), slot, -1)
    below = structure_second - limit
    low_marks = jnp.where(above, -1, below // GRAIN * CAP + ranks_second)
    low_match = jnp.arange(low_slots, dtype=jnp.int32)[:, None] == low_marks[None, :]
    low_rows = jnp.max(jnp.where(low_match, below[None, :], -1), axis=1)

    take_first = one_hot(row_marks_first, row_slots)
    take_second = one_hot(
        jnp.where(above, row_marks_second, row_slots + low_marks), row_slots + low_slots
    )
    part_first = product(take_first, whole_first)
    part_second = product(take_second, whole_second)
    part_first = part_first.reshape(row_slots, first, halves, height).transpose(0, 2, 1, 3)
    part_first = part_first.reshape(row_slots * first, width)
    part_second = part_second.reshape(row_slots + low_slots, second, halves, height)
    part_second = part_second.transpose(0, 2, 1, 3)
    part_second = part_second.reshape((row_slots + low_slots) * second, width)
    spread = lax.all_gather(jnp.concatenate([part_first, part_second], axis=0), "col", axis=0)
    cut = part_first.shape[0]
    got_first = spread[:, :cut].reshape(cols, row_slots, halves, first, height)
    got_second = spread[:, cut:].reshape(cols, row_slots + low_slots, halves, second, height)
    got_first = got_first.transpose(1, 0, 2, 3, 4).reshape(row_slots, rows, first * height)
    got_second = got_second.transpose(1, 0, 2, 3, 4).reshape(-1, rows, second * height)
    upper_second = got_second[:row_slots]
    low_second = got_second[row_slots:].reshape(low_slots, second * TILE)

    flat = blocks.transpose(0, 2, 1, 3).reshape(tiles * height, tiles * width)
    kept_rows = jnp.concatenate(
        [
            local_rows(structure_first, row_marks_first, row_slots, height),
            local_rows(structure_second, row_marks_second, row_slots, height),
        ]
    )
    take_kept = (
        kept_rows[:, None] == jnp.arange(tiles * height, dtype=jnp.int32)[None, :]
    ).astype(jnp.float32)
    kept = product(take_kept, flat)

    place = jnp.arange(first * TILE, dtype=jnp.int32)
    place_row = place // (first * height)
    place_tile = place // height % first
    named = place_tile * TILE + place_row * height + place % height
    meet_low = (named[:, None] == low_rows[None, :]).astype(jnp.float32)
    first_at_low = product(got_first.reshape(row_slots, first * TILE), meet_low)
    folded = product(first_at_low, low_second).reshape(row_slots, rows, second * height)
    left = jnp.concatenate(
        [
            jnp.concatenate([got_first, -folded], axis=2),
            jnp.concatenate(
                [jnp.zeros((row_slots, rows, first * height), jnp.float32), upper_second], axis=2
            ),
        ],
        axis=0,
    )
    partial = product(left.reshape(2 * row_slots, every * TILE), kept, 0)
    partial = partial.reshape(rows, every * height, tiles * width)

    own_low = jnp.arange(first * height, dtype=jnp.int32)
    own_low = own_low // height * TILE + row_index * height + own_low % height
    own_meet = (own_low[:, None] == low_rows[None, :]).astype(jnp.float32)
    own_second = product(own_meet, low_second)
    flat_diag = first_diag.transpose(0, 2, 1, 3).reshape(first * height, first_width)
    low_partial = product(own_second, flat_diag, 0)
    low_partial = low_partial.reshape(rows, second * height, first_width)

    slabs = [low_partial[:, :, k * width : (k + 1) * width] for k in range(first)]
    slabs.append(jnp.zeros((rows, (every - first * second) * height, width), jnp.float32))
    joined = jnp.concatenate([partial, jnp.concatenate(slabs, axis=1)], axis=2)
    summed = lax.psum_scatter(joined, "row", scatter_dimension=0, tiled=False)
    image = summed[:, : tiles * width]
    step = second * height
    low_image = jnp.concatenate(
        [summed[k * step : (k + 1) * step, tiles * width :] for k in range(first)], axis=1
    )

    edge = first * height
    column_ids = jnp.arange(tiles * width, dtype=jnp.int32)
    col_rows_first = local_rows(structure_first, col_marks_first, col_slots, width)
    col_rows_second = local_rows(structure_second, col_marks_second, col_slots, width)
    pick_first = (column_ids[:, None] == col_rows_first[None, :]).astype(jnp.float32)
    pick_second = (column_ids[:, None] == col_rows_second[None, :]).astype(jnp.float32)
    picked = jnp.concatenate([product(image, pick_first), product(image[edge:], pick_second)], axis=0)
    met = lax.all_gather(picked, "col", axis=0)
    met = met.transpose(1, 0, 2).reshape(-1, cols * col_slots)
    dense_first = product(one_hot(all_marks_first, cols * col_slots), whole_first)
    dense_second = product(one_hot(all_marks_second, cols * col_slots), whole_second)
    corner = product(met[: every * height], dense_first)
    low_block = low_image - corner[edge:]
    low_all = lax.all_gather(low_block, "col", axis=0)
    low_all = low_all.transpose(1, 0, 2).reshape(second * height, first * TILE)
    spot = jnp.arange(first * TILE, dtype=jnp.int32)
    spot = spot // width % first * TILE + spot // first_width * width + spot % width
    below_marks = jnp.where(above, -1, below)
    dense_low = product(
        (spot[:, None] == below_marks[None, :]).astype(jnp.float32), whole_second
    )
    final = product(met[every * height :], dense_second) + product(low_all, dense_low)

    def tiled(matrix, up, across):
        return matrix.reshape(up, height, across, width).transpose(0, 2, 1, 3)

    row_first = jnp.concatenate(
        [-tiled(image[:edge], first, tiles), first_diag + tiled(corner[:edge], first, first)], axis=1
    )
    row_second = jnp.concatenate(
        [
            -tiled(image[edge:], second, tiles),
            -tiled(low_block, second, first),
            second_diag + tiled(final, second, second),
        ],
        axis=1,
    )
    return (close_packed(row_first), close_packed(row_second))

F32 = jnp.float32
BF16 = jnp.bfloat16
MESH = pl.DeviceIdType.MESH


def over(value, size):
    return lax.shift_right_logical(value, jnp.int32(size.bit_length() - 1))


def within(value, size):
    return value & jnp.int32(size - 1)


def iota(shape, dim):
    return lax.broadcasted_iota(jnp.int32, shape, dim)


def ones_at(mask):
    return jnp.where(mask, 1.0, 0.0).astype(BF16)


def dd(left, right, left_dim=1, right_dim=0):
    return lax.dot_general(
        left, right, (((left_dim,), (right_dim,)), ((), ())), preferred_element_type=F32
    )


def halves_of(value):
    high = value.astype(BF16)
    return high, (value - high.astype(F32)).astype(BF16)


def three(left, right):
    return dd(left[0], right[0]) + dd(left[0], right[1]) + dd(left[1], right[0])


def grown(value, count):
    rest = count - value.shape[0]
    return jnp.concatenate([value, jnp.zeros((rest, value.shape[1]), value.dtype)], axis=0)


def spots(hits, places):
    return jnp.max(jnp.where(hits, places, -1.0), axis=1, keepdims=True)


def fused(dims, names, *refs):
    ref = dict(zip(names, refs))
    rows, cols, height, width, tiles, first, entries = dims
    chunks = first + 1
    shard = entries // rows
    wide = tiles * width
    tall = tiles * height
    row_slots = tall // GRAIN * CAP
    low_slots = first * height // GRAIN * CAP
    col_slots = wide // GRAIN * CAP
    edge = first * height
    row_pad = -(-row_slots // 128) * 128
    col_pad = -(-col_slots // 128) * 128
    half = height // 2

    r = lax.axis_index("row")
    c = lax.axis_index("col")
    core = r % 2
    chip = r // 2
    chip_x = chip % 2
    chip_y = chip // 2
    by_x = r + 2 - 4 * chip_x
    by_y = r + 4 - 8 * chip_y
    by_both = r + 6 - 4 * chip_x - 8 * chip_y
    mate = r + 1 - 2 * core
    peers = {1: by_x, 2: by_y, 3: by_both}

    def chip_at(rel):
        x = 1 - chip_x if rel % 2 else chip_x
        y = 1 - chip_y if rel // 2 else chip_y
        return y * 2 + x

    sent = []

    def remote(source, target, send, recv, device, column=None):
        return pltpu.make_async_remote_copy(
            src_ref=source,
            dst_ref=target,
            send_sem=send,
            recv_sem=recv,
            device_id=(device, c if column is None else column),
            device_id_type=MESH,
        )

    def launch(copy):
        copy.start()
        sent.append((None, copy))
        return copy

    barrier = pltpu.get_barrier_semaphore()
    for peer in (mate, by_x, by_y, by_both):
        pl.semaphore_signal(barrier, inc=1, device_id=(peer, c), device_id_type=MESH)
    for step in range(1, cols):
        other = (c + step) % cols
        pl.semaphore_signal(barrier, inc=1, device_id=(r, other), device_id_type=MESH)
    pl.semaphore_wait(barrier, 4 + cols - 1)

    panel = ref["panel"]
    pall = ref["pall"]

    def own_rows(device):
        return pl.ds(pl.multiple_of(device * shard, 8), shard)

    gather = {}
    for k in range(chunks):
        for rel, peer in peers.items():
            gather[k, rel] = launch(
                remote(
                    panel.at[k],
                    pall.at[k, own_rows(r)],
                    ref["g_send"].at[k, rel],
                    ref["g_recv"].at[k, rel],
                    peer,
                )
            )
        gather[k, 0] = launch(
            remote(
                panel.at[k],
                pall.at[k, own_rows(r)],
                ref["g_send"].at[k, 0],
                ref["g_recv"].at[k, 0],
                mate,
            )
        )
    for k in range(chunks):
        pall[k, own_rows(r), :] = panel[k]

    def ranks(row, which):
        group = over(row, GRAIN)
        at = iota((1, entries), 1)

        def step(b, total):
            start = pl.multiple_of(b * 128, 128)
            column = over(ref["scol"][pl.ds(start, 128), which : which + 1], GRAIN)
            order = iota((128, 1), 0) + b * 128
            hit = (column == group) & (order < at)
            return total + jnp.sum(jnp.where(hit, 1.0, 0.0), axis=0, keepdims=True)

        total = lax.fori_loop(0, entries // 128, step, jnp.zeros((1, entries), F32))
        return total.astype(jnp.int32)

    def owned(row, rank, size):
        owner = over(within(row, TILE), size)
        group = over(row, TILE) * (size // GRAIN) + over(within(row, size), GRAIN)
        place = over(row, TILE) * size + within(row, size)
        return owner, group * CAP + rank, place.astype(F32)

    row1 = ref["srow"][0:1, :]
    row2 = ref["srow"][1:2, :]
    rank1 = ranks(row1, 0)
    rank2 = ranks(row2, 1)
    above = row2 < tiles * TILE
    r_owner1, r_slot1, r_place1 = owned(row1, rank1, height)
    r_owner2, r_slot2, r_place2 = owned(row2, rank2, height)
    c_owner1, c_slot1, c_place1 = owned(row1, rank1, width)
    c_owner2, c_slot2, c_place2 = owned(row2, rank2, width)
    mark1 = jnp.where(r_owner1 == r, r_slot1, -1)
    mark2 = jnp.where(r_owner2 == r, r_slot2, -1)
    upper2 = jnp.where(above, mark2, -1)
    lower2 = jnp.where(above | (r_owner2 != r), -1, r_slot2 - row_slots)

    def keep(at, marks, places):
        spot = spots(iota((row_pad, entries), 0) == marks, places)
        take = ones_at(spot == iota((row_pad, tall), 1).astype(F32))

        def step(j, carry):
            block = ref["ancestor"][:, pl.ds(j, 1), :, :].reshape(tall, width)
            high, low = halves_of(block)
            span = pl.ds(pl.multiple_of(j * width, 128), width)
            ref["kept_h"][at, :, span] = dd(take, high).astype(BF16)
            ref["kept_l"][at, :, span] = dd(take, low).astype(BF16)
            return carry

        lax.fori_loop(0, tiles, step, 0)

    keep(0, mark1, r_place1)

    def z_step(d, at, sends, recvs):
        for way, sign in ((0, 1), (1, -1)):
            q = c - d * sign
            have = (q >= 0) & (q < cols)
            more = (c + sign >= 0) & (c + sign < cols)

            def act(q=q, way=way, sign=sign, more=more):
                copy = remote(at(q), at(q), sends.at[d, way], recvs.at[q], r, c + sign)
                if d:
                    copy.wait_recv()

                @pl.when(more)
                def _():
                    copy.start()

            if d:
                pl.when(have)(act)
            else:
                act()

    def z_drain(at, sends, recvs):
        for d in range(cols - 1):
            for way, sign in ((0, 1), (1, -1)):
                q = c - d * sign
                go = (q >= 0) & (q < cols) & (c + sign >= 0) & (c + sign < cols)

                @pl.when(go)
                def _(q=q, way=way, sign=sign):
                    remote(at(q), at(q), sends.at[d, way], recvs.at[q], r, c + sign).wait_send()

    def v_at(k):
        if k < first:
            return (lambda q: ref["v_one"].at[k, q]), ref["v_send"].at[k], ref["v_recv"].at[k]
        return (lambda q: ref["v_two"].at[q]), ref["v_send"].at[k], ref["v_recv"].at[k]

    one_rows = ref["v_one"].shape[2]
    two_rows = ref["v_two"].shape[1]
    take1 = ones_at(iota((one_rows, entries), 0) == mark1)
    for k in range(chunks):
        for rel in (1, 2, 3):
            gather[k, rel].wait_recv()
            peer = peers[rel]
            part = pall.at[k, own_rows(peer)]
            gather[k, 3 + rel] = launch(
                remote(part, part, ref["g_send"].at[k, 3 + rel], ref["g_recv"].at[k, 3 + rel], mate)
            )
        for rel in (0, 4, 5, 6):
            gather[k, rel].wait_recv()
        high, low = halves_of(pall[k])
        span = slice(k * width, (k + 1) * width)
        ref["ph"][:, span] = high
        ref["pl"][:, span] = low
        take = take1 if k < first else ones_at(iota((two_rows, entries), 0) == mark2)
        picked = dd(take, high) + dd(take, low)
        if k < first:
            ref["v_one"][k, pl.ds(c, 1)] = picked[None]
        else:
            ref["v_two"][pl.ds(c, 1)] = picked[None]
        z_step(0, *v_at(k))

    keep(1, upper2, r_place2)
    low_spot = spots(iota((128, entries), 0) == lower2, r_place2 - float(tall))
    spread_low = ones_at(low_spot == iota((128, edge), 1).astype(F32))

    def sizes(k):
        return wide if k < first else wide + first * width

    block = width * 3 if tiles % 3 == 0 else width

    def unit(k, rel):
        klass = chip_at(rel)
        buf = ref[f"z{k}"]
        if k < first:
            value = ref["v_one"][k, pl.ds(klass, 1)].reshape(one_rows, width)[:row_slots]
        else:
            both = ref["v_two"][pl.ds(klass, 1)].reshape(two_rows, width)
            value = both[:row_slots]
            under = halves_of(grown(both[row_slots : row_slots + low_slots], 128).T)
            under = halves_of(dd(under[0], spread_low) + dd(under[1], spread_low))
        turned = halves_of(grown(value, row_pad).T)
        at = 0 if k < first else 1

        def step(j, carry):
            span = pl.ds(pl.multiple_of(j * block, 128), block)
            kept = (ref["kept_h"][at, :, span], ref["kept_l"][at, :, span])
            out = three(turned, kept)
            if k >= first:
                out = out - three(under, (ref["y_h"][:edge, span], ref["y_l"][:edge, span]))
            buf[rel, 0, :, span] = out[:height]
            buf[rel, 1, :, span] = out[height:]
            return carry

        lax.fori_loop(0, wide // block, step, 0)
        if k >= first:
            out = three(under, (ref["d_h"][...], ref["d_l"][...]))
            buf[rel, 0, :, wide:] = out[:height]
            buf[rel, 1, :, wide:] = out[height:]
        return launch(
            remote(
                buf.at[rel, 1 - core],
                ref[f"m{k}"].at[rel],
                ref["r_send"].at[k, rel],
                ref["r_recv"].at[k, rel],
                mate,
            )
        )

    def strips(count, body):
        def step(i, carry):
            body(pl.multiple_of(i * 8, 8))
            return carry

        lax.fori_loop(0, count // 8, step, 0)

    def begin(k):
        swaps = {rel: unit(k, rel) for rel in (3, 1, 2, 0)}
        total = ref[f"t{k}"]
        buf = ref[f"z{k}"]
        got = ref[f"m{k}"]
        live = {}

        def pair(rel):
            swaps[rel].wait_recv()

            def body(i):
                at = pl.ds(i, 8)
                mine = buf[rel, pl.ds(core, 1), at, :].reshape(8, sizes(k))
                total[rel, at, :] = mine + got[rel, at, :]

            strips(height, body)

        def pass_on(index, source, target, peer):
            live[index] = launch(
                remote(source, target, ref["r_send"].at[k, index], ref["r_recv"].at[k, index], peer)
            )

        lower = pl.ds(0, half)
        upper = pl.ds(half, half)
        pair(3)
        pass_on(4, total.at[3, lower], ref[f"i{k}"].at[0], by_x)
        pass_on(5, total.at[3, upper], ref[f"i{k}"].at[1], by_y)
        pair(1)
        pass_on(6, total.at[1, lower], ref[f"f{k}"].at[0], by_x)
        pair(2)
        pass_on(7, total.at[2, upper], ref[f"f{k}"].at[1], by_y)
        return swaps, live, pass_on

    def middle(k, state):
        swaps, live, pass_on = state
        total = ref[f"t{k}"]
        live[5].wait_recv()

        def body(i):
            at = pl.ds(pl.multiple_of(i + half, 8), 8)
            total[1, at, :] = total[1, at, :] + ref[f"i{k}"][1, pl.ds(i, 8), :]

        strips(half, body)
        pass_on(8, total.at[1, pl.ds(half, half)], ref[f"f{k}"].at[2], by_x)
        live[4].wait_recv()

        def body(i):
            at = pl.ds(i, 8)
            total[2, at, :] = total[2, at, :] + ref[f"i{k}"][0, at, :]

        strips(half, body)
        pass_on(9, total.at[2, pl.ds(0, half)], ref[f"f{k}"].at[3], by_y)

    def finish(k, state):
        swaps, live, pass_on = state
        swaps[0].wait_recv()
        for index in (6, 7, 8, 9):
            live[index].wait_recv()
        buf = ref[f"z{k}"]
        got = ref[f"m{k}"]
        fin = ref[f"f{k}"]
        out = ref[f"t{k}"]
        for start, one, two in ((0, 0, 3), (half, 1, 2)):

            def body(i, start=start, one=one, two=two):
                at = pl.ds(pl.multiple_of(i + start, 8), 8)
                own = buf[0, pl.ds(core, 1), at, :].reshape(8, sizes(k)) + got[0, at, :]
                out[0, at, :] = own + (fin[one, pl.ds(i, 8), :] + fin[two, pl.ds(i, 8), :])

            strips(half, body)

        rows_at = pl.ds(k * height, height)

        def step(j, carry):
            span = pl.ds(pl.multiple_of(j * width, 128), width)
            tile = out[0, :, span]
            high, low = halves_of(tile)
            ref["y_h"][rows_at, span] = high
            ref["y_l"][rows_at, span] = low
            if k < first:
                ref["out_one"][k, pl.ds(j, 1)] = -tile[None]
            else:
                ref["out_two"][0, pl.ds(j, 1)] = -tile[None]
            return carry

        lax.fori_loop(0, tiles, step, 0)

    for k in range(first):
        for kk in range(first):
            high, low = halves_of(ref["diag_one"][k, kk])
            ref["d_h"][k * height : (k + 1) * height, kk * width : (kk + 1) * width] = high
            ref["d_l"][k * height : (k + 1) * height, kk * width : (kk + 1) * width] = low

    def arrive(at, steps):
        for d in steps:
            z_step(d, *at)

    every = range(1, cols)
    states = []
    for k in range(first):
        arrive(v_at(k), every)
        states.append(begin(k))
        middle(k, states[k])
    arrive(v_at(first), every)
    for k in range(first):
        finish(k, states[k])

    def picker(owner, slot, place, extra=None):
        mine = owner == c
        if extra is not None:
            mine = mine & extra
        spot = spots(iota((col_slots, entries), 0) == jnp.where(mine, slot, -1), place)
        return ones_at(spot == iota((col_slots, wide), 1).astype(F32))

    ref["pick"][0] = picker(c_owner1, c_slot1, c_place1)
    ref["pick"][1] = picker(c_owner2, c_slot2, c_place2, above)

    def s_at(n):
        return (lambda q: ref["s"].at[n, q]), ref["s_send"].at[n], ref["s_recv"].at[n]

    pick1 = ref["pick"][0]
    chosen = dd(pick1, ref["y_h"][:edge], 1, 1) + dd(pick1, ref["y_l"][:edge], 1, 1)
    ref["s"][0, pl.ds(c, 1)] = chosen[None]
    z_step(0, *s_at(0))
    last = begin(first)
    z_step(1, *s_at(0))

    def order_one(q, carry):
        take = ones_at(iota((col_pad, entries), 0) == jnp.where(c_owner1 == q, c_slot1, -1))
        ref["c1_h"][pl.ds(q, 1)] = dd(take, ref["ph"][:, : first * width]).astype(BF16)[None]
        ref["c1_l"][pl.ds(q, 1)] = dd(take, ref["pl"][:, : first * width]).astype(BF16)[None]
        return carry

    lax.fori_loop(0, cols, order_one, 0)
    middle(first, last)
    z_step(2, *s_at(0))

    def order_two(q, carry):
        mark = jnp.where((c_owner2 == q) & above, c_slot2, -1)
        take = ones_at(iota((col_pad, entries), 0) == mark)
        ref["c2_h"][pl.ds(q, 1)] = dd(take, ref["ph"][:, first * width :]).astype(BF16)[None]
        ref["c2_l"][pl.ds(q, 1)] = dd(take, ref["pl"][:, first * width :]).astype(BF16)[None]
        place = (over(row2, TILE) - tiles) * width + within(row2, width)
        mark = jnp.where((c_owner2 != q) | above, -1, place)
        take = ones_at(iota((first * width, entries), 0) == mark)
        ref["cl_h"][pl.ds(q, 1)] = dd(take, ref["ph"][:, first * width :]).astype(BF16)[None]
        ref["cl_l"][pl.ds(q, 1)] = dd(take, ref["pl"][:, first * width :]).astype(BF16)[None]
        return carry

    lax.fori_loop(0, cols, order_two, 0)
    finish(first, last)
    tail_h = ref["y_h"][edge:]
    tail_l = ref["y_l"][edge:]
    none = jnp.zeros_like(tail_h)
    pick1 = ref["pick"][0]
    pick2 = ref["pick"][1]
    chosen = (
        dd(pick1, jnp.concatenate([tail_h, none], axis=0), 1, 1)
        + dd(pick1, jnp.concatenate([tail_l, none], axis=0), 1, 1)
        + dd(pick2, jnp.concatenate([none, tail_h], axis=0), 1, 1)
        + dd(pick2, jnp.concatenate([none, tail_l], axis=0), 1, 1)
    )
    ref["s"][1, pl.ds(c, 1)] = chosen[None]
    z_step(0, *s_at(1))
    z_step(3, *s_at(0)) if cols > 3 else None
    z_step(1, *s_at(1))

    def turned(n, q):
        return halves_of(grown(ref["s"][n, q], col_pad).T)

    corner = jnp.zeros((edge, first * width), F32)
    for q in range(cols):
        corner = corner + three(turned(0, q), (ref["c1_h"][q], ref["c1_l"][q]))
    for k in range(first):
        for kk in range(first):
            piece = corner[k * height : (k + 1) * height, kk * width : (kk + 1) * width]
            ref["out_one"][k, tiles + kk] = ref["diag_one"][k, kk] + piece
    arrive(s_at(1), range(2, cols))
    cross = jnp.zeros((2 * height, first * width), F32)
    final = jnp.zeros((2 * height, width), F32)
    for q in range(cols):
        both = turned(1, q)
        cross = cross + three(both, (ref["c1_h"][q], ref["c1_l"][q]))
        final = final + three(both, (ref["c2_h"][q], ref["c2_l"][q]))
    bottom = cross[:height] - ref[f"t{first}"][0, :, wide:]
    ref["b"][pl.ds(c, 1)] = bottom[None]
    ends = []
    for step in range(1, cols):
        other = (c + step) % cols
        ends.append(
            launch(
                remote(
                    ref["b"].at[c], ref["b"].at[c], ref["b_send"].at[step], ref["b_recv"].at[c], r, other
                )
            )
        )
    for kk in range(first):
        ref["out_two"][0, tiles + kk] = bottom[:, kk * width : (kk + 1) * width]
    for step in range(1, cols):
        other = (c + step) % cols
        remote(
            ref["b"].at[other], ref["b"].at[other], ref["b_send"].at[step], ref["b_recv"].at[other], r, other
        ).wait_recv()
    result = ref["diag_two"][0, 0] + final[height:]
    for q in range(cols):
        result = result - three(halves_of(ref["b"][q]), (ref["cl_h"][q], ref["cl_l"][q]))
    ref["out_two"][0, tiles + first] = result

    for _, copy in sent:
        copy.wait_send()
    for k in range(chunks):
        z_drain(*v_at(k))
    for n in range(2):
        z_drain(*s_at(n))


def on_device_fused(
    ancestor,
    inverse_first,
    panel_first,
    structure_first,
    inverse_second,
    panel_second,
    structure_second,
):
    rows = lax.axis_size("row")
    cols = lax.axis_size("col")
    height = TILE // rows
    width = TILE // cols
    tiles = ancestor.shape[0]
    first = inverse_first.shape[0]
    entries = structure_first.shape[0]
    chunks = first + 1
    wide = tiles * width
    tall = tiles * height
    row_slots = tall // GRAIN * CAP
    low_slots = first * height // GRAIN * CAP
    col_slots = wide // GRAIN * CAP
    row_pad = -(-row_slots // 128) * 128
    col_pad = -(-col_slots // 128) * 128
    one_rows = -(-row_slots // 16) * 16
    two_rows = -(-(row_slots + low_slots) // 16) * 16
    panel = jnp.concatenate([panel_first.transpose(1, 0, 2), panel_second.transpose(1, 0, 2)], axis=0)
    structure = jnp.stack([structure_first, structure_second])
    dma = pltpu.SemaphoreType.DMA
    scratch = {
        "pall": pltpu.VMEM((chunks, entries, width), F32),
        "ph": pltpu.VMEM((entries, chunks * width), BF16),
        "pl": pltpu.VMEM((entries, chunks * width), BF16),
        "kept_h": pltpu.VMEM((2, row_pad, wide), BF16),
        "kept_l": pltpu.VMEM((2, row_pad, wide), BF16),
        "v_one": pltpu.VMEM((first, cols, one_rows, width), F32),
        "v_two": pltpu.VMEM((cols, two_rows, width), F32),
        "y_h": pltpu.VMEM((chunks * height, wide), BF16),
        "y_l": pltpu.VMEM((chunks * height, wide), BF16),
        "d_h": pltpu.VMEM((first * height, first * width), BF16),
        "d_l": pltpu.VMEM((first * height, first * width), BF16),
        "pick": pltpu.VMEM((2, col_slots, wide), BF16),
        "s": pltpu.VMEM((2, cols, col_slots, 2 * height), F32),
        "c1_h": pltpu.VMEM((cols, col_pad, first * width), BF16),
        "c1_l": pltpu.VMEM((cols, col_pad, first * width), BF16),
        "c2_h": pltpu.VMEM((cols, col_pad, width), BF16),
        "c2_l": pltpu.VMEM((cols, col_pad, width), BF16),
        "cl_h": pltpu.VMEM((cols, first * width, width), BF16),
        "cl_l": pltpu.VMEM((cols, first * width, width), BF16),
        "b": pltpu.VMEM((cols, height, first * width), F32),
        "g_send": dma((chunks, 7)),
        "g_recv": dma((chunks, 7)),
        "v_send": dma((chunks, cols, 2)),
        "v_recv": dma((chunks, cols)),
        "r_send": dma((chunks, 10)),
        "r_recv": dma((chunks, 10)),
        "s_send": dma((2, cols, 2)),
        "s_recv": dma((2, cols)),
        "b_send": dma((cols,)),
        "b_recv": dma((cols,)),
    }
    for k in range(chunks):
        size = wide if k < first else wide + first * width
        scratch[f"z{k}"] = pltpu.VMEM((4, 2, height, size), F32)
        scratch[f"m{k}"] = pltpu.VMEM((4, height, size), F32)
        scratch[f"t{k}"] = pltpu.VMEM((4, height, size), F32)
        scratch[f"i{k}"] = pltpu.VMEM((2, height // 2, size), F32)
        scratch[f"f{k}"] = pltpu.VMEM((4, height // 2, size), F32)
    inputs = ["ancestor", "diag_one", "diag_two", "panel", "srow", "scol"]
    names = inputs + ["out_one", "out_two"] + list(scratch)
    vmem = pl.BlockSpec(memory_space=pltpu.VMEM)
    dims = (rows, cols, height, width, tiles, first, entries)
    return pl.pallas_call(
        functools.partial(fused, dims, names),
        out_shape=(
            jax.ShapeDtypeStruct((first, tiles + first, height, width), F32),
            jax.ShapeDtypeStruct((1, tiles + first + 1, height, width), F32),
        ),
        in_specs=[vmem] * len(inputs),
        out_specs=(vmem, vmem),
        scratch_shapes=list(scratch.values()),
        compiler_params=pltpu.CompilerParams(
            collective_id=0, has_side_effects=True, vmem_limit_bytes=60 * 1024 * 1024
        ),
    )(
        open_packed(ancestor, height, width),
        open_packed(inverse_first, height, width),
        open_packed(inverse_second, height, width),
        panel,
        structure,
        structure.T,
    )


def fits(rows, cols):
    return rows == 8 and rows == 2 * cols and TILE // cols % 128 == 0


def solution(mesh):
    body = on_device_fused if fits(mesh.shape["row"], mesh.shape["col"]) else on_device
    in_specs = (
        P(None, None, "row", "col"),
        P(None, None, "row", "col"),
        P("row", None, "col"),
        P(),
        P(None, None, "row", "col"),
        P("row", None, "col"),
        P(),
    )
    out_specs = (P(None, None, "row", "col"), P(None, None, "row", "col"))
    return jax.shard_map(
        body, mesh=mesh, in_specs=in_specs, out_specs=out_specs, check_vma=False
    )
```

```python
import functools

import jax
import jax.numpy as jnp
from jax import lax
from jax.experimental import pallas as pl
from jax.experimental.pallas import tpu as pltpu
from jax.sharding import PartitionSpec as P

TILE = 512
GRAIN = 16
CAP = 6


def open_packed(packed, row_height, col_width):
    return packed.reshape(packed.shape[0], packed.shape[1], row_height, col_width)


def close_packed(tiles):
    depth = tiles.shape[2] * tiles.shape[3] // 128
    return tiles.reshape(tiles.shape[0], tiles.shape[1], depth, 128)


def product(left, right, left_dim=1):
    return lax.dot_general(
        left,
        right,
        (((left_dim,), (0,)), ((), ())),
        precision=lax.Precision.HIGH,
        preferred_element_type=jnp.float32,
    )


def entry_ranks(structure):
    group = structure // GRAIN
    order = jnp.arange(structure.shape[0], dtype=jnp.int32)
    same = (group[:, None] == group[None, :]) & (order[None, :] < order[:, None])
    return jnp.sum(same.astype(jnp.int32), axis=1)


def slots_within(structure, ranks, height):
    owner = structure % TILE // height
    group = structure // TILE * (height // GRAIN) + structure % height // GRAIN
    return owner, group * CAP + ranks


def one_hot(marks, count):
    return (jnp.arange(count, dtype=jnp.int32)[:, None] == marks[None, :]).astype(jnp.float32)


def local_rows(structure, marks, count, height):
    row = structure // TILE * height + structure % height
    match = jnp.arange(count, dtype=jnp.int32)[:, None] == marks[None, :]
    return jnp.max(jnp.where(match, row[None, :], -1), axis=1)


def on_device(
    ancestor,
    inverse_first,
    panel_first,
    structure_first,
    inverse_second,
    panel_second,
    structure_second,
):
    rows = lax.axis_size("row")
    cols = lax.axis_size("col")
    height = TILE // rows
    width = TILE // cols
    halves = width // height
    row_index = lax.axis_index("row")
    col_index = lax.axis_index("col")
    blocks = open_packed(ancestor, height, width)
    first_diag = open_packed(inverse_first, height, width)
    second_diag = open_packed(inverse_second, height, width)
    tiles = blocks.shape[0]
    first = first_diag.shape[0]
    second = second_diag.shape[0]
    every = first + second
    limit = tiles * TILE
    first_width = first * width

    panels = jnp.concatenate(
        [panel_first.reshape(-1, first_width), panel_second.reshape(-1, second * width)], axis=1
    )
    both = lax.all_gather(panels, "row", axis=0, tiled=True)
    whole_first = both[:, :first_width]
    whole_second = both[:, first_width:]

    above = structure_second < limit
    ranks_first = entry_ranks(structure_first)
    ranks_second = entry_ranks(structure_second)
    row_slots = tiles * height // GRAIN * CAP
    col_slots = tiles * width // GRAIN * CAP
    low_slots = first * TILE // GRAIN * CAP
    owner, slot = slots_within(structure_first, ranks_first, height)
    row_marks_first = jnp.where(owner == row_index, slot, -1)
    owner, slot = slots_within(structure_second, ranks_second, height)
    row_marks_second = jnp.where(above & (owner == row_index), slot, -1)
    owner, slot = slots_within(structure_first, ranks_first, width)
    all_marks_first = owner * col_slots + slot
    col_marks_first = jnp.where(owner == col_index, slot, -1)
    owner, slot = slots_within(structure_second, ranks_second, width)
    all_marks_second = jnp.where(above, owner * col_slots + slot, -1)
    col_marks_second = jnp.where(above & (owner == col_index), slot, -1)
    below = structure_second - limit
    low_marks = jnp.where(above, -1, below // GRAIN * CAP + ranks_second)
    low_match = jnp.arange(low_slots, dtype=jnp.int32)[:, None] == low_marks[None, :]
    low_rows = jnp.max(jnp.where(low_match, below[None, :], -1), axis=1)

    take_first = one_hot(row_marks_first, row_slots)
    take_second = one_hot(
        jnp.where(above, row_marks_second, row_slots + low_marks), row_slots + low_slots
    )
    part_first = product(take_first, whole_first)
    part_second = product(take_second, whole_second)
    part_first = part_first.reshape(row_slots, first, halves, height).transpose(0, 2, 1, 3)
    part_first = part_first.reshape(row_slots * first, width)
    part_second = part_second.reshape(row_slots + low_slots, second, halves, height)
    part_second = part_second.transpose(0, 2, 1, 3)
    part_second = part_second.reshape((row_slots + low_slots) * second, width)
    spread = lax.all_gather(jnp.concatenate([part_first, part_second], axis=0), "col", axis=0)
    cut = part_first.shape[0]
    got_first = spread[:, :cut].reshape(cols, row_slots, halves, first, height)
    got_second = spread[:, cut:].reshape(cols, row_slots + low_slots, halves, second, height)
    got_first = got_first.transpose(1, 0, 2, 3, 4).reshape(row_slots, rows, first * height)
    got_second = got_second.transpose(1, 0, 2, 3, 4).reshape(-1, rows, second * height)
    upper_second = got_second[:row_slots]
    low_second = got_second[row_slots:].reshape(low_slots, second * TILE)

    flat = blocks.transpose(0, 2, 1, 3).reshape(tiles * height, tiles * width)
    kept_rows = jnp.concatenate(
        [
            local_rows(structure_first, row_marks_first, row_slots, height),
            local_rows(structure_second, row_marks_second, row_slots, height),
        ]
    )
    take_kept = (
        kept_rows[:, None] == jnp.arange(tiles * height, dtype=jnp.int32)[None, :]
    ).astype(jnp.float32)
    kept = product(take_kept, flat)

    place = jnp.arange(first * TILE, dtype=jnp.int32)
    place_row = place // (first * height)
    place_tile = place // height % first
    named = place_tile * TILE + place_row * height + place % height
    meet_low = (named[:, None] == low_rows[None, :]).astype(jnp.float32)
    first_at_low = product(got_first.reshape(row_slots, first * TILE), meet_low)
    folded = product(first_at_low, low_second).reshape(row_slots, rows, second * height)
    left = jnp.concatenate(
        [
            jnp.concatenate([got_first, -folded], axis=2),
            jnp.concatenate(
                [jnp.zeros((row_slots, rows, first * height), jnp.float32), upper_second], axis=2
            ),
        ],
        axis=0,
    )
    partial = product(left.reshape(2 * row_slots, every * TILE), kept, 0)
    partial = partial.reshape(rows, every * height, tiles * width)

    own_low = jnp.arange(first * height, dtype=jnp.int32)
    own_low = own_low // height * TILE + row_index * height + own_low % height
    own_meet = (own_low[:, None] == low_rows[None, :]).astype(jnp.float32)
    own_second = product(own_meet, low_second)
    flat_diag = first_diag.transpose(0, 2, 1, 3).reshape(first * height, first_width)
    low_partial = product(own_second, flat_diag, 0)
    low_partial = low_partial.reshape(rows, second * height, first_width)

    slabs = [low_partial[:, :, k * width : (k + 1) * width] for k in range(first)]
    slabs.append(jnp.zeros((rows, (every - first * second) * height, width), jnp.float32))
    joined = jnp.concatenate([partial, jnp.concatenate(slabs, axis=1)], axis=2)
    summed = lax.psum_scatter(joined, "row", scatter_dimension=0, tiled=False)
    image = summed[:, : tiles * width]
    step = second * height
    low_image = jnp.concatenate(
        [summed[k * step : (k + 1) * step, tiles * width :] for k in range(first)], axis=1
    )

    edge = first * height
    column_ids = jnp.arange(tiles * width, dtype=jnp.int32)
    col_rows_first = local_rows(structure_first, col_marks_first, col_slots, width)
    col_rows_second = local_rows(structure_second, col_marks_second, col_slots, width)
    pick_first = (column_ids[:, None] == col_rows_first[None, :]).astype(jnp.float32)
    pick_second = (column_ids[:, None] == col_rows_second[None, :]).astype(jnp.float32)
    picked = jnp.concatenate([product(image, pick_first), product(image[edge:], pick_second)], axis=0)
    met = lax.all_gather(picked, "col", axis=0)
    met = met.transpose(1, 0, 2).reshape(-1, cols * col_slots)
    dense_first = product(one_hot(all_marks_first, cols * col_slots), whole_first)
    dense_second = product(one_hot(all_marks_second, cols * col_slots), whole_second)
    corner = product(met[: every * height], dense_first)
    low_block = low_image - corner[edge:]
    low_all = lax.all_gather(low_block, "col", axis=0)
    low_all = low_all.transpose(1, 0, 2).reshape(second * height, first * TILE)
    spot = jnp.arange(first * TILE, dtype=jnp.int32)
    spot = spot // width % first * TILE + spot // first_width * width + spot % width
    below_marks = jnp.where(above, -1, below)
    dense_low = product(
        (spot[:, None] == below_marks[None, :]).astype(jnp.float32), whole_second
    )
    final = product(met[every * height :], dense_second) + product(low_all, dense_low)

    def tiled(matrix, up, across):
        return matrix.reshape(up, height, across, width).transpose(0, 2, 1, 3)

    row_first = jnp.concatenate(
        [-tiled(image[:edge], first, tiles), first_diag + tiled(corner[:edge], first, first)], axis=1
    )
    row_second = jnp.concatenate(
        [
            -tiled(image[edge:], second, tiles),
            -tiled(low_block, second, first),
            second_diag + tiled(final, second, second),
        ],
        axis=1,
    )
    return (close_packed(row_first), close_packed(row_second))

F32 = jnp.float32
BF16 = jnp.bfloat16
MESH = pl.DeviceIdType.MESH


def over(value, size):
    return lax.shift_right_logical(value, jnp.int32(size.bit_length() - 1))


def within(value, size):
    return value & jnp.int32(size - 1)


def iota(shape, dim):
    return lax.broadcasted_iota(jnp.int32, shape, dim)


def ones_at(mask):
    return jnp.where(mask, 1.0, 0.0).astype(BF16)


def dd(left, right, left_dim=1, right_dim=0):
    return lax.dot_general(
        left, right, (((left_dim,), (right_dim,)), ((), ())), preferred_element_type=F32
    )


def halves_of(value):
    high = value.astype(BF16)
    return high, (value - high.astype(F32)).astype(BF16)


def three(left, right):
    return dd(left[0], right[0]) + dd(left[0], right[1]) + dd(left[1], right[0])


def grown(value, count):
    rest = count - value.shape[0]
    return jnp.concatenate([value, jnp.zeros((rest, value.shape[1]), value.dtype)], axis=0)


def spots(hits, places):
    return jnp.max(jnp.where(hits, places, -1.0), axis=1, keepdims=True)


def fused(dims, names, *refs):
    ref = dict(zip(names, refs))
    rows, cols, height, width, tiles, first, entries, groups = dims
    chunks = first + 1
    shard = entries // rows
    wide = tiles * width
    tall = tiles * height
    row_slots = tall // GRAIN * CAP
    low_slots = first * height // GRAIN * CAP
    tile_slots = width // GRAIN * CAP
    col_slots = tiles * tile_slots
    edge = first * height
    fringe = first * width
    row_pad = -(-row_slots // 128) * 128
    col_pad = -(-col_slots // 128) * 128
    half = height // 2

    r = lax.axis_index("row")
    c = lax.axis_index("col")
    core = r % 2
    chip = r // 2
    chip_x = chip % 2
    chip_y = chip // 2
    by_x = r + 2 - 4 * chip_x
    by_y = r + 4 - 8 * chip_y
    by_both = r + 6 - 4 * chip_x - 8 * chip_y
    mate = r + 1 - 2 * core
    peers = {3: by_both, 1: by_x, 2: by_y}

    def chip_at(rel):
        x = 1 - chip_x if rel % 2 else chip_x
        y = 1 - chip_y if rel // 2 else chip_y
        return y * 2 + x

    sent = []
    drains = []

    def remote(source, target, send, recv, device, column=None):
        return pltpu.make_async_remote_copy(
            src_ref=source,
            dst_ref=target,
            send_sem=send,
            recv_sem=recv,
            device_id=(device, c if column is None else column),
            device_id_type=MESH,
        )

    def launch(copy):
        copy.start()
        sent.append(copy)
        return copy

    barrier = pltpu.get_barrier_semaphore()
    for peer in (mate, by_x, by_y, by_both):
        pl.semaphore_signal(barrier, inc=1, device_id=(peer, c), device_id_type=MESH)
    for step in range(1, cols):
        other = (c + step) % cols
        pl.semaphore_signal(barrier, inc=1, device_id=(r, other), device_id_type=MESH)
    loads = []
    for index, (source, target) in enumerate(
        (("ancestor", "a"), ("diag_one", "d_one"), ("diag_two", "d_two"))
    ):
        loads.append(pltpu.make_async_copy(ref[source], ref[target], ref["l_sem"].at[index]))
        loads[-1].start()

    def ranks(row):
        group = over(row, GRAIN)
        total = [jnp.zeros((1, 128), F32) for _ in range(entries // 128)]
        lanes = iota((128, 128), 1)
        order = iota((128, 128), 0)
        for b in range(entries // 128):
            one = group[:, b * 128 : (b + 1) * 128]
            column = jnp.broadcast_to(one, (128, 128)).T
            for t in range(b, entries // 128):
                hit = column == group[:, t * 128 : (t + 1) * 128]
                if t == b:
                    hit = hit & (order < lanes)
                total[t] = total[t] + jnp.sum(jnp.where(hit, 1.0, 0.0), axis=0, keepdims=True)
        return jnp.concatenate(total, axis=1).astype(jnp.int32)

    def owned(row, rank, size):
        owner = over(within(row, TILE), size)
        group = over(row, TILE) * (size // GRAIN) + over(within(row, size), GRAIN)
        place = over(row, TILE) * size + within(row, size)
        return owner, group * CAP + rank, place.astype(F32)

    row1 = ref["list_one"][...].reshape(1, entries)
    row2 = ref["list_two"][...].reshape(1, entries)
    rank1 = ranks(row1)
    rank2 = ranks(row2)
    above = row2 < tiles * TILE
    r_owner1, r_slot1, r_place1 = owned(row1, rank1, height)
    r_owner2, r_slot2, r_place2 = owned(row2, rank2, height)
    c_owner1, c_slot1, c_place1 = owned(row1, rank1, width)
    c_owner2, c_slot2, c_place2 = owned(row2, rank2, width)
    mark1 = jnp.where(r_owner1 == r, r_slot1, -1)
    mark2 = jnp.where(r_owner2 == r, r_slot2, -1)
    upper2 = jnp.where(above, mark2, -1)
    lower2 = jnp.where(above | (r_owner2 != r), -1, r_slot2 - row_slots)

    pl.semaphore_wait(barrier, 4 + cols - 1)
    pall = ref["pall"]

    def own_rows(device):
        return pl.ds(pl.multiple_of(device * shard, 8), shard)

    def panel(k):
        return ref["panel_one"].at[k] if k < first else ref["panel_two"].at[k - first]

    gather = {}
    for k in range(chunks):
        for rel, peer in (*peers.items(), (0, mate)):
            gather[k, rel] = launch(
                remote(
                    panel(k),
                    pall.at[k, own_rows(r)],
                    ref["g_send"].at[k, rel],
                    ref["g_recv"].at[k, rel],
                    peer,
                )
            )
    for k in range(chunks):
        pall[k, own_rows(r), :] = panel(k)[...]

    def keep(at, marks, places):
        spot = spots(iota((row_pad, entries), 0) == marks, places)
        take = ones_at(spot == iota((row_pad, tall), 1).astype(F32))

        def step(j, carry):
            block = ref["a"][:, pl.ds(j, 1), :, :].reshape(tall, width)
            high, low = halves_of(block)
            span = pl.ds(pl.multiple_of(j * width, 128), width)
            ref["kept_h"][at, :, span] = dd(take, high).astype(BF16)
            ref["kept_l"][at, :, span] = dd(take, low).astype(BF16)
            return carry

        lax.fori_loop(0, tiles, step, 0)

    def spread(at, sends, recvs):
        for index, (sign, reach) in enumerate(((1, 2), (-1, 2), (1, 1), (-1, 1))):
            there = c + sign * reach
            go = (there >= 0) & (there < cols)

            def copy(there=there, index=index):
                return remote(at(c), at(c), sends.at[index], recvs.at[c], r, there)

            @pl.when(go)
            def _(copy=copy):
                copy().start()

            drains.append((go, copy))

    def forward(at, sends, recvs):
        for index, sign in ((4, 1), (5, -1)):
            q = c - 2 * sign
            there = c + sign
            go = (q >= 0) & (q < cols) & (there >= 0) & (there < cols)

            def copy(q=q, there=there, index=index):
                return remote(at(q), at(q), sends.at[index], recvs.at[q], r, there)

            @pl.when(go)
            def _(copy=copy):
                copy().wait_recv()
                copy().start()

            drains.append((go, copy))

    def arrive(at, sends, recvs):
        for reach in range(1, cols):
            for sign in (1, -1):
                q = c - reach * sign
                there = c + sign
                go = (q >= 0) & (q < cols)
                if reach == 2:
                    go = go & ((there < 0) | (there >= cols))

                @pl.when(go)
                def _(q=q):
                    remote(at(q), at(q), sends.at[0], recvs.at[q], r, c).wait_recv()

    def v_at(k):
        if k < first:
            return (lambda q: ref["v_one"].at[k, q]), ref["v_send"].at[k], ref["v_recv"].at[k]
        return (lambda q: ref["v_two"].at[q]), ref["v_send"].at[k], ref["v_recv"].at[k]

    one_rows = -(-row_slots // 16) * 16
    two_rows = -(-(row_slots + low_slots) // 16) * 16
    take1 = ones_at(iota((one_rows, entries), 0) == mark1)
    loads[0].wait()
    keep(0, mark1, r_place1)
    for k in range(chunks):
        for rel in (1, 2, 3):
            gather[k, rel].wait_recv()
            part = pall.at[k, own_rows(peers[rel])]
            gather[k, 3 + rel] = launch(
                remote(part, part, ref["g_send"].at[k, 3 + rel], ref["g_recv"].at[k, 3 + rel], mate)
            )
        for rel in (0, 4, 5, 6):
            gather[k, rel].wait_recv()
        high, low = halves_of(pall[k])
        span = slice(k * width, (k + 1) * width)
        ref["ph"][:, span] = high
        ref["pl"][:, span] = low
        take = take1 if k < first else ones_at(iota((two_rows, entries), 0) == mark2)
        picked = dd(take, high) + dd(take, low)
        if k < first:
            ref["v_one"][k, pl.ds(c, 1)] = picked[None, :row_slots]
        else:
            ref["v_two"][pl.ds(c, 1)] = picked[None, : row_slots + low_slots]
        spread(*v_at(k))
        if k:
            forward(*v_at(k - 1))

    keep(1, upper2, r_place2)
    low_spot = spots(iota((128, entries), 0) == lower2, r_place2 - float(tall))
    spread_low = ones_at(low_spot == iota((128, edge), 1).astype(F32))
    for load in loads[1:]:
        load.wait()
    for k in range(first):
        for kk in range(first):
            high, low = halves_of(ref["d_one"][k, kk])
            ref["d_h"][k * height : (k + 1) * height, kk * width : (kk + 1) * width] = high
            ref["d_l"][k * height : (k + 1) * height, kk * width : (kk + 1) * width] = low

    def picker(which, owner, slot, place, extra=None):
        mine = owner == c
        if extra is not None:
            mine = mine & extra
        spot = spots(iota((col_slots, entries), 0) == jnp.where(mine, slot, -1), place)
        for start, stop in groups:
            span = slice(start * tile_slots, stop * tile_slots)
            count = (stop - start) * width
            here = iota(((stop - start) * tile_slots, count), 1) + start * width
            ref["pick"][which, span, :count] = ones_at(spot[span] == here.astype(F32))

    picker(0, c_owner1, c_slot1, c_place1)
    picker(1, c_owner2, c_slot2, c_place2, above)

    def ready(k):
        arrive(*v_at(k))
        for rel in range(4):
            klass = chip_at(rel)
            if k < first:
                value = ref["v_one"][k, pl.ds(klass, 1)].reshape(row_slots, width)
            else:
                both = ref["v_two"][pl.ds(klass, 1)].reshape(row_slots + low_slots, width)
                value = both[:row_slots]
                under = halves_of(grown(both[row_slots:], 128).T)
                under = halves_of(dd(under[0], spread_low) + dd(under[1], spread_low))
                for n in range(2):
                    start = (4 * n + rel) * width
                    ref["under"][start : start + width, :] = under[n]
            turned = halves_of(grown(value, row_pad).T)
            for n in range(2):
                start = (4 * n + rel) * width
                ref["turned"][k, start : start + width, :] = turned[n]

    def stacked(left, high, low):
        count = left.shape[0] // 2
        both = dd(left, high)
        return both[:count] + both[count:] + dd(left[:count], low)

    stages = [(k, g) for g in range(len(groups)) for k in range(first)]
    stages += [(first, g) for g in range(len(groups))]
    names_of = {stage: s for s, stage in enumerate(stages)}
    live = {}

    def put(s, part, start, stop):
        for rel in range(4):
            for side in range(2):
                top = rel * width + side * height
                ref[f"z{s}"][side, rel, :, start:stop] = part[top : top + height]

    def begin(s):
        k, g = stages[s]
        start, stop = groups[g]
        span = slice(start * width, stop * width)
        count = (stop - start) * width
        at = 0 if k < first else 1
        part = stacked(ref["turned"][k], ref["kept_h"][at, :, span], ref["kept_l"][at, :, span])
        if k >= first:
            part = part - stacked(ref["under"][...], ref["y_h"][:edge, span], ref["y_l"][:edge, span])
        put(s, part, 0, count)
        if k >= first and g == len(groups) - 1:
            part = stacked(ref["under"][...], ref["d_h"][...], ref["d_l"][...])
            put(s, part, count, count + fringe)
        live[s, 0] = launch(
            remote(
                ref[f"z{s}"].at[1 - core],
                ref[f"m{s}"],
                ref["r_send"].at[s, 0],
                ref["r_recv"].at[s, 0],
                mate,
            )
        )

    def strips(count, body):
        def step(i, carry):
            body(pl.multiple_of(i * 8, 8))
            return carry

        lax.fori_loop(0, count // 8, step, 0)

    def pass_on(s, index, source, target, peer):
        live[s, index] = launch(
            remote(source, target, ref["r_send"].at[s, index], ref["r_recv"].at[s, index], peer)
        )

    lower = pl.ds(0, half)
    upper = pl.ds(half, half)

    def push(s):
        live[s, 0].wait_recv()
        total = ref[f"t{s}"]
        got = ref[f"m{s}"]
        own = ref[f"z{s}"]
        count = total.shape[2]

        def pair(rel):
            def body(i):
                at = pl.ds(i, 8)
                mine = own[pl.ds(core, 1), rel, at, :].reshape(8, count)
                total[rel, at, :] = mine + got[rel, at, :]

            strips(height, body)

        pair(3)
        pass_on(s, 1, total.at[3, lower], ref[f"i{s}"].at[0], by_x)
        pass_on(s, 2, total.at[3, upper], ref[f"i{s}"].at[1], by_y)
        pair(1)
        pass_on(s, 3, total.at[1, lower], ref[f"f{s}"].at[0], by_x)
        pair(2)
        pass_on(s, 4, total.at[2, upper], ref[f"f{s}"].at[1], by_y)
        pair(0)

    def middle(s):
        total = ref[f"t{s}"]
        live[s, 2].wait_recv()

        def body(i):
            at = pl.ds(pl.multiple_of(i + half, 8), 8)
            total[1, at, :] = total[1, at, :] + ref[f"i{s}"][1, pl.ds(i, 8), :]

        strips(half, body)
        pass_on(s, 5, total.at[1, upper], ref[f"f{s}"].at[2], by_x)
        live[s, 1].wait_recv()

        def body(i):
            at = pl.ds(i, 8)
            total[2, at, :] = total[2, at, :] + ref[f"i{s}"][0, at, :]

        strips(half, body)
        pass_on(s, 6, total.at[2, lower], ref[f"f{s}"].at[3], by_y)

    writes = []

    def write(source, target):
        copy = pltpu.make_async_copy(source, target, ref["w_sem"].at[len(writes)])
        copy.start()
        writes.append(copy)

    def s_at(n, g):
        start, stop = groups[g]
        span = pl.ds(start * tile_slots, (stop - start) * tile_slots)
        return (lambda q: ref["s"].at[n, q, span]), ref["s_send"].at[n, g], ref["s_recv"].at[n, g]

    def choose(n, g):
        start, stop = groups[g]
        span = slice(start * tile_slots, stop * tile_slots)
        count = (stop - start) * width
        columns = slice(start * width, stop * width)
        pick1 = ref["pick"][0, span, :count]
        if n == 0:
            chosen = dd(pick1, ref["y_h"][:edge, columns], 1, 1)
            chosen = chosen + dd(pick1, ref["y_l"][:edge, columns], 1, 1)
        else:
            pick2 = ref["pick"][1, span, :count]
            high = ref["y_h"][edge:, columns]
            low = ref["y_l"][edge:, columns]
            none = jnp.zeros_like(high)
            chosen = (
                dd(pick1, jnp.concatenate([high, none], axis=0), 1, 1)
                + dd(pick1, jnp.concatenate([low, none], axis=0), 1, 1)
                + dd(pick2, jnp.concatenate([none, high], axis=0), 1, 1)
                + dd(pick2, jnp.concatenate([none, low], axis=0), 1, 1)
            )
        ref["s"][n, pl.ds(c, 1), span, :] = chosen[None]
        spread(*s_at(n, g))

    done = set()

    def finish(s):
        k, g = stages[s]
        start, stop = groups[g]
        for index in (3, 4, 5, 6):
            live[s, index].wait_recv()
        fin = ref[f"f{s}"]
        out = ref[f"t{s}"]
        for base, one, two in ((0, 0, 3), (half, 1, 2)):

            def body(i, base=base, one=one, two=two):
                at = pl.ds(pl.multiple_of(i + base, 8), 8)
                out[0, at, :] = out[0, at, :] + (fin[one, pl.ds(i, 8), :] + fin[two, pl.ds(i, 8), :])

            strips(half, body)
        count = (stop - start) * width
        span = slice(start * width, stop * width)
        high, low = halves_of(out[0, :, :count])
        ref["y_h"][k * height : (k + 1) * height, span] = high
        ref["y_l"][k * height : (k + 1) * height, span] = low
        into, at, target = ("o_one", k, "out_one") if k < first else ("o_two", 0, "out_two")
        for j in range(start, stop):
            ref[into][at, j] = -out[0, :, (j - start) * width : (j + 1 - start) * width]
        write(ref[into].at[at, start:stop], ref[target].at[at, start:stop])
        done.add(s)
        if k >= first:
            choose(1, g)
            return (1, g)
        if all(names_of[other, g] in done for other in range(first)):
            choose(0, g)
            return (0, g)
        return None

    def order_one(q):
        take = ones_at(iota((col_pad, entries), 0) == jnp.where(c_owner1 == q, c_slot1, -1))
        ref["c1_h"][q] = dd(take, ref["ph"][:, :fringe]).astype(BF16)
        ref["c1_l"][q] = dd(take, ref["pl"][:, :fringe]).astype(BF16)

    def order_two(q):
        mark = jnp.where((c_owner2 == q) & above, c_slot2, -1)
        place = (over(row2, TILE) - tiles) * width + within(row2, width)
        mark = jnp.where((c_owner2 == q) & (row2 >= tiles * TILE), col_pad + place, mark)
        take = ones_at(iota((col_pad + fringe, entries), 0) == mark)
        high = dd(take, ref["ph"][:, fringe:]).astype(BF16)
        low = dd(take, ref["pl"][:, fringe:]).astype(BF16)
        ref["c2_h"][q] = high[:col_pad]
        ref["c2_l"][q] = low[:col_pad]
        ref["cl_h"][q] = high[col_pad:]
        ref["cl_l"][q] = low[col_pad:]

    aside = [lambda: forward(*v_at(first))]
    aside += [lambda q=q: order_one(q) for q in range(cols)]
    aside += [lambda q=q: order_two(q) for q in range(cols)]
    pending = []
    begun = set()

    def settle(s, now):
        if s not in done:
            piece = finish(s)
            if piece is not None:
                pending.append((now + 2, piece))

    for step in range(len(stages) + 3):
        if step >= 3:
            settle(step - 3, step)
        if step < len(stages):
            k, g = stages[step]
            if k not in begun:
                begun.add(k)
                ready(k)
            if k >= first:
                for other in range(first):
                    settle(names_of[other, g], step)
            begin(step)
        if aside:
            aside.pop(0)()
        if step < len(stages):
            push(step)
        if 2 <= step < len(stages) + 2:
            middle(step - 2)
        while pending and pending[0][0] <= step:
            forward(*s_at(*pending.pop(0)[1]))
    for work in aside:
        work()
    for _, piece in pending:
        forward(*s_at(*piece))

    def turned(n, q):
        return halves_of(grown(ref["s"][n, q], col_pad).T)

    for g in range(len(groups)):
        arrive(*s_at(0, g))
    corner = jnp.zeros((edge, fringe), F32)
    for q in range(cols):
        corner = corner + three(turned(0, q), (ref["c1_h"][q], ref["c1_l"][q]))
    for k in range(first):
        for kk in range(first):
            piece = corner[k * height : (k + 1) * height, kk * width : (kk + 1) * width]
            ref["o_one"][k, tiles + kk] = ref["d_one"][k, kk] + piece
        write(ref["o_one"].at[k, tiles:], ref["out_one"].at[k, tiles:])
    for g in range(len(groups)):
        arrive(*s_at(1, g))
    cross = jnp.zeros((2 * height, fringe), F32)
    final = jnp.zeros((2 * height, width), F32)
    for q in range(cols):
        both = turned(1, q)
        cross = cross + three(both, (ref["c1_h"][q], ref["c1_l"][q]))
        final = final + three(both, (ref["c2_h"][q], ref["c2_l"][q]))
    tail = ref[f"t{len(stages) - 1}"]
    bottom = cross[:height] - tail[0, :, tail.shape[2] - fringe :]
    ref["b"][pl.ds(c, 1)] = bottom[None]
    for step in range(1, cols):
        other = (c + step) % cols
        launch(
            remote(
                ref["b"].at[c], ref["b"].at[c], ref["b_send"].at[step], ref["b_recv"].at[c], r, other
            )
        )
    for kk in range(first):
        ref["o_two"][0, tiles + kk] = bottom[:, kk * width : (kk + 1) * width]
    for step in range(1, cols):
        other = (c + step) % cols
        remote(
            ref["b"].at[other], ref["b"].at[other], ref["b_send"].at[step], ref["b_recv"].at[other], r, other
        ).wait_recv()
    result = ref["d_two"][0, 0] + final[height:]
    for q in range(cols):
        result = result - three(halves_of(ref["b"][q]), (ref["cl_h"][q], ref["cl_l"][q]))
    ref["o_two"][0, tiles + first] = result
    write(ref["o_two"].at[0, tiles:], ref["out_two"].at[0, tiles:])

    for copy in sent:
        copy.wait_send()
    for go, copy in drains:

        @pl.when(go)
        def _(copy=copy):
            copy().wait_send()

    for copy in writes:
        copy.wait()


def on_device_fused(
    ancestor,
    inverse_first,
    panel_first,
    structure_first,
    inverse_second,
    panel_second,
    structure_second,
):
    rows = lax.axis_size("row")
    cols = lax.axis_size("col")
    height = TILE // rows
    width = TILE // cols
    tiles = ancestor.shape[0]
    first = inverse_first.shape[0]
    entries = structure_first.shape[0]
    chunks = first + 1
    wide = tiles * width
    row_slots = tiles * height // GRAIN * CAP
    low_slots = first * height // GRAIN * CAP
    col_slots = wide // GRAIN * CAP
    row_pad = -(-row_slots // 128) * 128
    col_pad = -(-col_slots // 128) * 128
    edge = first * height
    fringe = first * width
    parts = min(3, tiles)
    groups = [(i * tiles // parts, (i + 1) * tiles // parts) for i in range(parts)]
    widest = max(stop - start for start, stop in groups) * width
    stages = chunks * parts
    dma = pltpu.SemaphoreType.DMA
    scratch = {
        "a": pltpu.VMEM((tiles, tiles, height, width), F32),
        "d_one": pltpu.VMEM((first, first, height, width), F32),
        "d_two": pltpu.VMEM((1, 1, height, width), F32),
        "o_one": pltpu.VMEM((first, tiles + first, height, width), F32),
        "o_two": pltpu.VMEM((1, tiles + first + 1, height, width), F32),
        "pall": pltpu.VMEM((chunks, entries, width), F32),
        "ph": pltpu.VMEM((entries, chunks * width), BF16),
        "pl": pltpu.VMEM((entries, chunks * width), BF16),
        "kept_h": pltpu.VMEM((2, row_pad, wide), BF16),
        "kept_l": pltpu.VMEM((2, row_pad, wide), BF16),
        "v_one": pltpu.VMEM((first, cols, row_slots, width), F32),
        "v_two": pltpu.VMEM((cols, row_slots + low_slots, width), F32),
        "turned": pltpu.VMEM((chunks, 8 * width, row_pad), BF16),
        "under": pltpu.VMEM((8 * width, edge), BF16),
        "y_h": pltpu.VMEM((chunks * height, wide), BF16),
        "y_l": pltpu.VMEM((chunks * height, wide), BF16),
        "d_h": pltpu.VMEM((edge, fringe), BF16),
        "d_l": pltpu.VMEM((edge, fringe), BF16),
        "pick": pltpu.VMEM((2, col_slots, widest), BF16),
        "s": pltpu.VMEM((2, cols, col_slots, 2 * height), F32),
        "c1_h": pltpu.VMEM((cols, col_pad, fringe), BF16),
        "c1_l": pltpu.VMEM((cols, col_pad, fringe), BF16),
        "c2_h": pltpu.VMEM((cols, col_pad, width), BF16),
        "c2_l": pltpu.VMEM((cols, col_pad, width), BF16),
        "cl_h": pltpu.VMEM((cols, fringe, width), BF16),
        "cl_l": pltpu.VMEM((cols, fringe, width), BF16),
        "b": pltpu.VMEM((cols, height, fringe), F32),
        "l_sem": dma((3,)),
        "w_sem": dma((stages + first + 1,)),
        "g_send": dma((chunks, 7)),
        "g_recv": dma((chunks, 7)),
        "v_send": dma((chunks, 6)),
        "v_recv": dma((chunks, cols)),
        "r_send": dma((stages, 7)),
        "r_recv": dma((stages, 7)),
        "s_send": dma((2, parts, 6)),
        "s_recv": dma((2, parts, cols)),
        "b_send": dma((cols,)),
        "b_recv": dma((cols,)),
    }
    for s in range(stages):
        k, g = (first, s - first * parts) if s >= first * parts else (s % first, s // first)
        size = (groups[g][1] - groups[g][0]) * width
        if s == stages - 1:
            size += fringe
        scratch[f"z{s}"] = pltpu.VMEM((2, 4, height, size), F32)
        scratch[f"m{s}"] = pltpu.VMEM((4, height, size), F32)
        scratch[f"t{s}"] = pltpu.VMEM((4, height, size), F32)
        scratch[f"i{s}"] = pltpu.VMEM((2, height // 2, size), F32)
        scratch[f"f{s}"] = pltpu.VMEM((4, height // 2, size), F32)
    inputs = ["ancestor", "diag_one", "diag_two", "panel_one", "panel_two", "list_one", "list_two"]
    names = inputs + ["out_one", "out_two"] + list(scratch)
    vmem = pl.BlockSpec(memory_space=pltpu.VMEM)
    hbm = pl.BlockSpec(memory_space=pl.ANY)
    dims = (rows, cols, height, width, tiles, first, entries, groups)
    return pl.pallas_call(
        functools.partial(fused, dims, names),
        out_shape=(
            jax.ShapeDtypeStruct((first, tiles + first, height, width), F32),
            jax.ShapeDtypeStruct((1, tiles + first + 1, height, width), F32),
        ),
        in_specs=[hbm] * 3 + [vmem] * 4,
        out_specs=(hbm, hbm),
        scratch_shapes=list(scratch.values()),
        compiler_params=pltpu.CompilerParams(
            collective_id=0, has_side_effects=True, vmem_limit_bytes=60 * 1024 * 1024
        ),
    )(
        open_packed(ancestor, height, width),
        open_packed(inverse_first, height, width),
        open_packed(inverse_second, height, width),
        panel_first.transpose(1, 0, 2),
        panel_second.transpose(1, 0, 2),
        structure_first,
        structure_second,
    )


def fits(rows, cols):
    return rows == 8 and rows == 2 * cols and TILE // cols % 128 == 0


def solution(mesh):
    body = on_device_fused if fits(mesh.shape["row"], mesh.shape["col"]) else on_device
    in_specs = (
        P(None, None, "row", "col"),
        P(None, None, "row", "col"),
        P("row", None, "col"),
        P(),
        P(None, None, "row", "col"),
        P("row", None, "col"),
        P(),
    )
    out_specs = (P(None, None, "row", "col"), P(None, None, "row", "col"))
    return jax.shard_map(
        body, mesh=mesh, in_specs=in_specs, out_specs=out_specs, check_vma=False
    )
```

```python
import functools

import jax
import jax.numpy as jnp
from jax import lax
from jax.experimental import pallas as pl
from jax.experimental.pallas import tpu as pltpu
from jax.sharding import PartitionSpec as P

TILE = 512
GRAIN = 16
CAP = 6


def open_packed(packed, row_height, col_width):
    return packed.reshape(packed.shape[0], packed.shape[1], row_height, col_width)


def close_packed(tiles):
    depth = tiles.shape[2] * tiles.shape[3] // 128
    return tiles.reshape(tiles.shape[0], tiles.shape[1], depth, 128)


def product(left, right, left_dim=1):
    return lax.dot_general(
        left,
        right,
        (((left_dim,), (0,)), ((), ())),
        precision=lax.Precision.HIGH,
        preferred_element_type=jnp.float32,
    )


def entry_ranks(structure):
    group = structure // GRAIN
    order = jnp.arange(structure.shape[0], dtype=jnp.int32)
    same = (group[:, None] == group[None, :]) & (order[None, :] < order[:, None])
    return jnp.sum(same.astype(jnp.int32), axis=1)


def slots_within(structure, ranks, height):
    owner = structure % TILE // height
    group = structure // TILE * (height // GRAIN) + structure % height // GRAIN
    return owner, group * CAP + ranks


def one_hot(marks, count):
    return (jnp.arange(count, dtype=jnp.int32)[:, None] == marks[None, :]).astype(jnp.float32)


def local_rows(structure, marks, count, height):
    row = structure // TILE * height + structure % height
    match = jnp.arange(count, dtype=jnp.int32)[:, None] == marks[None, :]
    return jnp.max(jnp.where(match, row[None, :], -1), axis=1)


def on_device(
    ancestor,
    inverse_first,
    panel_first,
    structure_first,
    inverse_second,
    panel_second,
    structure_second,
):
    rows = lax.axis_size("row")
    cols = lax.axis_size("col")
    height = TILE // rows
    width = TILE // cols
    halves = width // height
    row_index = lax.axis_index("row")
    col_index = lax.axis_index("col")
    blocks = open_packed(ancestor, height, width)
    first_diag = open_packed(inverse_first, height, width)
    second_diag = open_packed(inverse_second, height, width)
    tiles = blocks.shape[0]
    first = first_diag.shape[0]
    second = second_diag.shape[0]
    every = first + second
    limit = tiles * TILE
    first_width = first * width

    panels = jnp.concatenate(
        [panel_first.reshape(-1, first_width), panel_second.reshape(-1, second * width)], axis=1
    )
    both = lax.all_gather(panels, "row", axis=0, tiled=True)
    whole_first = both[:, :first_width]
    whole_second = both[:, first_width:]

    above = structure_second < limit
    ranks_first = entry_ranks(structure_first)
    ranks_second = entry_ranks(structure_second)
    row_slots = tiles * height // GRAIN * CAP
    col_slots = tiles * width // GRAIN * CAP
    low_slots = first * TILE // GRAIN * CAP
    owner, slot = slots_within(structure_first, ranks_first, height)
    row_marks_first = jnp.where(owner == row_index, slot, -1)
    owner, slot = slots_within(structure_second, ranks_second, height)
    row_marks_second = jnp.where(above & (owner == row_index), slot, -1)
    owner, slot = slots_within(structure_first, ranks_first, width)
    all_marks_first = owner * col_slots + slot
    col_marks_first = jnp.where(owner == col_index, slot, -1)
    owner, slot = slots_within(structure_second, ranks_second, width)
    all_marks_second = jnp.where(above, owner * col_slots + slot, -1)
    col_marks_second = jnp.where(above & (owner == col_index), slot, -1)
    below = structure_second - limit
    low_marks = jnp.where(above, -1, below // GRAIN * CAP + ranks_second)
    low_match = jnp.arange(low_slots, dtype=jnp.int32)[:, None] == low_marks[None, :]
    low_rows = jnp.max(jnp.where(low_match, below[None, :], -1), axis=1)

    take_first = one_hot(row_marks_first, row_slots)
    take_second = one_hot(
        jnp.where(above, row_marks_second, row_slots + low_marks), row_slots + low_slots
    )
    part_first = product(take_first, whole_first)
    part_second = product(take_second, whole_second)
    part_first = part_first.reshape(row_slots, first, halves, height).transpose(0, 2, 1, 3)
    part_first = part_first.reshape(row_slots * first, width)
    part_second = part_second.reshape(row_slots + low_slots, second, halves, height)
    part_second = part_second.transpose(0, 2, 1, 3)
    part_second = part_second.reshape((row_slots + low_slots) * second, width)
    spread = lax.all_gather(jnp.concatenate([part_first, part_second], axis=0), "col", axis=0)
    cut = part_first.shape[0]
    got_first = spread[:, :cut].reshape(cols, row_slots, halves, first, height)
    got_second = spread[:, cut:].reshape(cols, row_slots + low_slots, halves, second, height)
    got_first = got_first.transpose(1, 0, 2, 3, 4).reshape(row_slots, rows, first * height)
    got_second = got_second.transpose(1, 0, 2, 3, 4).reshape(-1, rows, second * height)
    upper_second = got_second[:row_slots]
    low_second = got_second[row_slots:].reshape(low_slots, second * TILE)

    flat = blocks.transpose(0, 2, 1, 3).reshape(tiles * height, tiles * width)
    kept_rows = jnp.concatenate(
        [
            local_rows(structure_first, row_marks_first, row_slots, height),
            local_rows(structure_second, row_marks_second, row_slots, height),
        ]
    )
    take_kept = (
        kept_rows[:, None] == jnp.arange(tiles * height, dtype=jnp.int32)[None, :]
    ).astype(jnp.float32)
    kept = product(take_kept, flat)

    place = jnp.arange(first * TILE, dtype=jnp.int32)
    place_row = place // (first * height)
    place_tile = place // height % first
    named = place_tile * TILE + place_row * height + place % height
    meet_low = (named[:, None] == low_rows[None, :]).astype(jnp.float32)
    first_at_low = product(got_first.reshape(row_slots, first * TILE), meet_low)
    folded = product(first_at_low, low_second).reshape(row_slots, rows, second * height)
    left = jnp.concatenate(
        [
            jnp.concatenate([got_first, -folded], axis=2),
            jnp.concatenate(
                [jnp.zeros((row_slots, rows, first * height), jnp.float32), upper_second], axis=2
            ),
        ],
        axis=0,
    )
    partial = product(left.reshape(2 * row_slots, every * TILE), kept, 0)
    partial = partial.reshape(rows, every * height, tiles * width)

    own_low = jnp.arange(first * height, dtype=jnp.int32)
    own_low = own_low // height * TILE + row_index * height + own_low % height
    own_meet = (own_low[:, None] == low_rows[None, :]).astype(jnp.float32)
    own_second = product(own_meet, low_second)
    flat_diag = first_diag.transpose(0, 2, 1, 3).reshape(first * height, first_width)
    low_partial = product(own_second, flat_diag, 0)
    low_partial = low_partial.reshape(rows, second * height, first_width)

    slabs = [low_partial[:, :, k * width : (k + 1) * width] for k in range(first)]
    slabs.append(jnp.zeros((rows, (every - first * second) * height, width), jnp.float32))
    joined = jnp.concatenate([partial, jnp.concatenate(slabs, axis=1)], axis=2)
    summed = lax.psum_scatter(joined, "row", scatter_dimension=0, tiled=False)
    image = summed[:, : tiles * width]
    step = second * height
    low_image = jnp.concatenate(
        [summed[k * step : (k + 1) * step, tiles * width :] for k in range(first)], axis=1
    )

    edge = first * height
    column_ids = jnp.arange(tiles * width, dtype=jnp.int32)
    col_rows_first = local_rows(structure_first, col_marks_first, col_slots, width)
    col_rows_second = local_rows(structure_second, col_marks_second, col_slots, width)
    pick_first = (column_ids[:, None] == col_rows_first[None, :]).astype(jnp.float32)
    pick_second = (column_ids[:, None] == col_rows_second[None, :]).astype(jnp.float32)
    picked = jnp.concatenate([product(image, pick_first), product(image[edge:], pick_second)], axis=0)
    met = lax.all_gather(picked, "col", axis=0)
    met = met.transpose(1, 0, 2).reshape(-1, cols * col_slots)
    dense_first = product(one_hot(all_marks_first, cols * col_slots), whole_first)
    dense_second = product(one_hot(all_marks_second, cols * col_slots), whole_second)
    corner = product(met[: every * height], dense_first)
    low_block = low_image - corner[edge:]
    low_all = lax.all_gather(low_block, "col", axis=0)
    low_all = low_all.transpose(1, 0, 2).reshape(second * height, first * TILE)
    spot = jnp.arange(first * TILE, dtype=jnp.int32)
    spot = spot // width % first * TILE + spot // first_width * width + spot % width
    below_marks = jnp.where(above, -1, below)
    dense_low = product(
        (spot[:, None] == below_marks[None, :]).astype(jnp.float32), whole_second
    )
    final = product(met[every * height :], dense_second) + product(low_all, dense_low)

    def tiled(matrix, up, across):
        return matrix.reshape(up, height, across, width).transpose(0, 2, 1, 3)

    row_first = jnp.concatenate(
        [-tiled(image[:edge], first, tiles), first_diag + tiled(corner[:edge], first, first)], axis=1
    )
    row_second = jnp.concatenate(
        [
            -tiled(image[edge:], second, tiles),
            -tiled(low_block, second, first),
            second_diag + tiled(final, second, second),
        ],
        axis=1,
    )
    return (close_packed(row_first), close_packed(row_second))

F32 = jnp.float32
BF16 = jnp.bfloat16
MESH = pl.DeviceIdType.MESH


def over(value, size):
    return lax.shift_right_logical(value, jnp.int32(size.bit_length() - 1))


def within(value, size):
    return value & jnp.int32(size - 1)


def iota(shape, dim):
    return lax.broadcasted_iota(jnp.int32, shape, dim)


def ones_at(mask):
    return jnp.where(mask, 1.0, 0.0).astype(BF16)


def dd(left, right, left_dim=1, right_dim=0):
    return lax.dot_general(
        left, right, (((left_dim,), (right_dim,)), ((), ())), preferred_element_type=F32
    )


def halves_of(value):
    high = value.astype(BF16)
    return high, (value - high.astype(F32)).astype(BF16)


def three(left, right):
    return dd(left[0], right[0]) + dd(left[0], right[1]) + dd(left[1], right[0])


def grown(value, count):
    rest = count - value.shape[0]
    if not rest:
        return value
    return jnp.concatenate([value, jnp.zeros((rest, value.shape[1]), value.dtype)], axis=0)


def spots(hits, places):
    return jnp.max(jnp.where(hits, places, -1.0), axis=1, keepdims=True)


def order_of(first, parts):
    return [(k, g) for k in range(first + 1) for g in range(parts)]


def fused(dims, names, *refs):
    ref = dict(zip(names, refs))
    rows, cols, height, width, tiles, first, entries, groups = dims
    chunks = first + 1
    shard = entries // rows
    wide = tiles * width
    tall = tiles * height
    row_slots = tall // GRAIN * CAP
    low_slots = first * height // GRAIN * CAP
    tile_slots = width // GRAIN * CAP
    col_slots = tiles * tile_slots
    edge = first * height
    fringe = first * width
    row_pad = -(-row_slots // 128) * 128
    half = height // 2

    r = lax.axis_index("row")
    c = lax.axis_index("col")
    core = r % 2
    chip = r // 2
    chip_x = chip % 2
    chip_y = chip // 2
    by_x = r + 2 - 4 * chip_x
    by_y = r + 4 - 8 * chip_y
    by_both = r + 6 - 4 * chip_x - 8 * chip_y
    mate = r + 1 - 2 * core
    peers = {3: by_both, 1: by_x, 2: by_y}

    def chip_at(rel):
        x = 1 - chip_x if rel % 2 else chip_x
        y = 1 - chip_y if rel // 2 else chip_y
        return y * 2 + x

    ends = []

    def remote(source, target, send, recv, device, column=None):
        return pltpu.make_async_remote_copy(
            src_ref=source,
            dst_ref=target,
            send_sem=send,
            recv_sem=recv,
            device_id=(device, c if column is None else column),
            device_id_type=MESH,
        )

    def launch(copy):
        copy.start()
        return copy

    def sent(whole, sem, go=None):
        ends.append((go, lambda: remote(whole(), whole(), sem, sem, mate).wait_send()))

    barrier = pltpu.get_barrier_semaphore()
    for peer in (mate, by_x, by_y, by_both):
        pl.semaphore_signal(barrier, inc=1, device_id=(peer, c), device_id_type=MESH)
    for step in range(1, cols):
        other = (c + step) % cols
        pl.semaphore_signal(barrier, inc=1, device_id=(r, other), device_id_type=MESH)
    loads = {}

    def load(name, source, target):
        loads[name] = pltpu.make_async_copy(source, target, ref["l_sem"].at[len(loads)])
        loads[name].start()

    load("list_one", ref["list_one"], ref["l_one"])
    load("list_two", ref["list_two"], ref["l_two"])
    for k in range(chunks):
        source = ref["panel_one"].at[:, k] if k < first else ref["panel_two"].at[:, k - first]
        load(k, source, ref["own"].at[k])
    load("a", ref["ancestor"], ref["a"])
    load("d_one", ref["diag_one"], ref["d_one"])
    load("d_two", ref["diag_two"], ref["d_two"])

    def ranks(row):
        group = over(row, GRAIN)
        total = [jnp.zeros((1, 128), F32) for _ in range(entries // 128)]
        lanes = iota((128, 128), 1)
        order = iota((128, 128), 0)
        for b in range(entries // 128):
            one = group[:, b * 128 : (b + 1) * 128]
            column = jnp.broadcast_to(one, (128, 128)).T
            for t in range(b, entries // 128):
                hit = column == group[:, t * 128 : (t + 1) * 128]
                if t == b:
                    hit = hit & (order < lanes)
                total[t] = total[t] + jnp.sum(jnp.where(hit, 1.0, 0.0), axis=0, keepdims=True)
        return jnp.concatenate(total, axis=1).astype(jnp.int32)

    def owned(row, rank, size):
        owner = over(within(row, TILE), size)
        group = over(row, TILE) * (size // GRAIN) + over(within(row, size), GRAIN)
        place = over(row, TILE) * size + within(row, size)
        return owner, group * CAP + rank, place.astype(F32)

    loads["list_one"].wait()
    loads["list_two"].wait()
    row1 = ref["l_one"][...].reshape(1, entries)
    row2 = ref["l_two"][...].reshape(1, entries)
    rank1 = ranks(row1)
    rank2 = ranks(row2)
    above = row2 < tiles * TILE
    r_owner1, r_slot1, r_place1 = owned(row1, rank1, height)
    r_owner2, r_slot2, r_place2 = owned(row2, rank2, height)
    c_owner1, c_slot1, c_place1 = owned(row1, rank1, width)
    c_owner2, c_slot2, c_place2 = owned(row2, rank2, width)
    mark1 = jnp.where(r_owner1 == r, r_slot1, -1)
    mark2 = jnp.where(r_owner2 == r, r_slot2, -1)
    upper2 = jnp.where(above, mark2, -1)
    lower2 = jnp.where(above | (r_owner2 != r), -1, r_slot2 - row_slots)

    pl.semaphore_wait(barrier, 4 + cols - 1)
    pall = ref["pall"]

    def own_rows(device):
        return pl.ds(pl.multiple_of(device * shard, 8), shard)

    gather = {}
    for k in range(chunks):
        loads[k].wait()
        for rel, peer in (*peers.items(), (0, mate)):
            gather[k, rel] = launch(
                remote(
                    ref["own"].at[k],
                    pall.at[k, own_rows(r)],
                    ref["g_send"].at[k],
                    ref["g_recv"].at[k, rel],
                    peer,
                )
            )
        sent(lambda k=k: pall.at[k, pl.ds(0, 7 * shard)], ref["g_send"].at[k])
    for k in range(chunks):
        pall[k, own_rows(r), :] = ref["own"][k]

    def keep(at, marks, places):
        spot = spots(iota((row_pad, entries), 0) == marks, places)
        take = ones_at(spot == iota((row_pad, tall), 1).astype(F32))

        def step(j, carry):
            block = ref["a"][:, pl.ds(j, 1), :, :].reshape(tall, width)
            high, low = halves_of(block)
            span = pl.ds(pl.multiple_of(j * width, 128), width)
            ref["kept_h"][at, :, span] = dd(take, high).astype(BF16)
            ref["kept_l"][at, :, span] = dd(take, low).astype(BF16)
            return carry

        lax.fori_loop(0, tiles, step, 0)

    def spread(at, sends, recvs, whole, direct=False):
        for sign, reach in ((1, 3), (-1, 3), (1, 2), (-1, 2), (1, 1), (-1, 1)):
            there = c + sign * reach
            if reach < cols - 1 or direct:

                @pl.when((there >= 0) & (there < cols))
                def _(there=there):
                    remote(at(c), at(c), sends, recvs.at[c], r, there).start()

        if direct:
            sent(lambda: whole(cols - 1), sends)
        else:
            edge_of = (c == 0) | (c == cols - 1)
            sent(lambda: whole(2), sends, edge_of)
            sent(lambda: whole(4), sends, jnp.logical_not(edge_of))

    def forward(at, sends, recvs, whole, direct=False):
        if direct:
            return
        for sign in (1, -1):
            q = c - 2 * sign
            there = c + sign

            @pl.when((q >= 0) & (q < cols) & (there >= 0) & (there < cols))
            def _(q=q, there=there):
                copy = remote(at(q), at(q), sends, recvs.at[q], r, there)
                copy.wait_recv()
                copy.start()

    def arrive(at, sends, recvs, whole, direct=False):
        for reach in range(1, cols):
            for sign in (1, -1):
                q = c - reach * sign
                there = c + sign
                go = (q >= 0) & (q < cols)
                if reach == 2 and not direct:
                    go = go & ((there < 0) | (there >= cols))

                @pl.when(go)
                def _(q=q):
                    remote(at(q), at(q), sends, recvs.at[q], r, c).wait_recv()

    def v_at(k):
        buf = ref["v_one"].at[k] if k < first else ref["v_two"]
        return buf.at.__getitem__, ref["v_send"].at[k], ref["v_recv"].at[k], lambda n: buf.at[pl.ds(0, n)]

    one_rows = -(-row_slots // 16) * 16
    two_rows = -(-(row_slots + low_slots) // 16) * 16
    take1 = ones_at(iota((one_rows, entries), 0) == mark1)
    loads["a"].wait()
    keep(0, mark1, r_place1)
    for k in range(chunks):
        for rel in (1, 2, 3):
            gather[k, rel].wait_recv()
            part = pall.at[k, own_rows(peers[rel])]
            gather[k, 3 + rel] = launch(
                remote(part, part, ref["g_send"].at[k], ref["g_recv"].at[k, 0], mate)
            )
        four = pall.at[k, pl.ds(0, 4 * shard)]
        remote(four, four, ref["g_send"].at[k], ref["g_recv"].at[k, 0], mate).wait_recv()
        high, low = halves_of(pall[k])
        span = slice(k * width, (k + 1) * width)
        ref["ph"][:, span] = high
        ref["pl"][:, span] = low
        take = take1 if k < first else ones_at(iota((two_rows, entries), 0) == mark2)
        picked = dd(take, high) + dd(take, low)
        if k < first:
            ref["v_one"][k, pl.ds(c, 1)] = picked[None, :row_slots]
        else:
            ref["v_two"][pl.ds(c, 1)] = picked[None, : row_slots + low_slots]
        spread(*v_at(k))
        if k:
            forward(*v_at(k - 1))

    keep(1, upper2, r_place2)
    low_spot = spots(iota((128, entries), 0) == lower2, r_place2 - float(tall))
    spread_low = ones_at(low_spot == iota((128, edge), 1).astype(F32))
    loads["d_one"].wait()
    loads["d_two"].wait()
    for k in range(first):
        for kk in range(first):
            high, low = halves_of(ref["d_one"][k, kk])
            ref["d_h"][k * height : (k + 1) * height, kk * width : (kk + 1) * width] = high
            ref["d_l"][k * height : (k + 1) * height, kk * width : (kk + 1) * width] = low

    def picker(which, owner, slot, place, extra=None):
        mine = owner == c
        if extra is not None:
            mine = mine & extra
        spot = spots(iota((col_slots, entries), 0) == jnp.where(mine, slot, -1), place)
        for start, stop in groups:
            span = slice(start * tile_slots, stop * tile_slots)
            count = (stop - start) * width
            here = iota(((stop - start) * tile_slots, count), 1) + start * width
            ref["pick"][which, span, :count] = ones_at(spot[span] == here.astype(F32))

    picker(0, c_owner1, c_slot1, c_place1)
    picker(1, c_owner2, c_slot2, c_place2, above)

    def ready(k):
        arrive(*v_at(k))
        for rel in range(4):
            klass = chip_at(rel)
            if k < first:
                value = ref["v_one"][k, pl.ds(klass, 1)].reshape(row_slots, width)
            else:
                both = ref["v_two"][pl.ds(klass, 1)].reshape(row_slots + low_slots, width)
                value = both[:row_slots]
                under = halves_of(grown(both[row_slots:], 128).T)
                under = halves_of(dd(under[0], spread_low) + dd(under[1], spread_low))
                for n in range(2):
                    start = (4 * n + rel) * width
                    ref["under"][start : start + width, :] = under[n]
            turned = halves_of(grown(value, row_pad).T)
            for n in range(2):
                start = (4 * n + rel) * width
                ref["turned"][k, start : start + width, :] = turned[n]

    def stacked(left, high, low):
        count = left.shape[0] // 2
        both = dd(left, high)
        return both[:count] + both[count:] + dd(left[:count], low)

    stages = order_of(first, len(groups))
    names_of = {stage: s for s, stage in enumerate(stages)}
    live = {}

    def put(s, part, start, stop):
        for rel in range(4):
            for side in range(2):
                top = rel * width + side * height
                ref[f"z{s}"][side * 4 + rel, :, start:stop] = part[top : top + height]

    def begin(s):
        k, g = stages[s]
        start, stop = groups[g]
        span = slice(start * width, stop * width)
        count = (stop - start) * width
        at = 0 if k < first else 1
        part = stacked(ref["turned"][k], ref["kept_h"][at, :, span], ref["kept_l"][at, :, span])
        if k >= first:
            part = part - stacked(ref["under"][...], ref["y_h"][:edge, span], ref["y_l"][:edge, span])
        put(s, part, 0, count)
        if k >= first and g == len(groups) - 1:
            part = stacked(ref["under"][...], ref["d_h"][...], ref["d_l"][...])
            put(s, part, count, count + fringe)
        live[s, 0] = launch(
            remote(
                ref[f"z{s}"].at[pl.ds((1 - core) * 4, 4)],
                ref[f"m{s}"],
                ref["r_send"].at[s],
                ref["r_recv"].at[s, 0],
                mate,
            )
        )
        sent(lambda: ref[f"z{s}"].at[pl.ds(0, 7)], ref["r_send"].at[s])

    def strips(count, body):
        def step(i, carry):
            body(pl.multiple_of(i * 8, 8))
            return carry

        lax.fori_loop(0, count // 8, step, 0)

    def pass_on(s, index, source, target, peer):
        live[s, index] = launch(
            remote(source, target, ref["r_send"].at[s], ref["r_recv"].at[s, min(index, 3)], peer)
        )

    lower = pl.ds(0, half)
    upper = pl.ds(half, half)

    def push(s):
        live[s, 0].wait_recv()
        total = ref[f"t{s}"]
        got = ref[f"m{s}"]
        own = ref[f"z{s}"]
        count = total.shape[2]

        def pair(rel):
            def body(i):
                at = pl.ds(i, 8)
                mine = own[pl.ds(core * 4 + rel, 1), at, :].reshape(8, count)
                total[rel, at, :] = mine + got[rel, at, :]

            strips(height, body)

        pair(3)
        pass_on(s, 1, total.at[3, lower], ref[f"i{s}"].at[0], by_x)
        pass_on(s, 2, total.at[3, upper], ref[f"i{s}"].at[1], by_y)
        pair(1)
        pass_on(s, 3, total.at[1, lower], ref[f"f{s}"].at[0], by_x)
        pair(2)
        pass_on(s, 4, total.at[2, upper], ref[f"f{s}"].at[1], by_y)
        pair(0)

    def middle(s):
        total = ref[f"t{s}"]
        live[s, 2].wait_recv()

        def body(i):
            at = pl.ds(pl.multiple_of(i + half, 8), 8)
            total[1, at, :] = total[1, at, :] + ref[f"i{s}"][1, pl.ds(i, 8), :]

        strips(half, body)
        pass_on(s, 5, total.at[1, upper], ref[f"f{s}"].at[2], by_x)
        live[s, 1].wait_recv()

        def body(i):
            at = pl.ds(i, 8)
            total[2, at, :] = total[2, at, :] + ref[f"i{s}"][0, at, :]

        strips(half, body)
        pass_on(s, 6, total.at[2, lower], ref[f"f{s}"].at[3], by_y)

    writes = []

    def write(source, target):
        copy = pltpu.make_async_copy(source, target, ref["w_sem"].at[len(writes)])
        copy.start()
        writes.append(copy)

    def counted(g):
        start, stop = groups[g]
        count = (stop - start) * tile_slots // 2
        return count, -(-count * cols // 128) * 128

    def s_at(n, g):
        buf = ref[f"s{n}{g}"]
        direct = n >= first and g == len(groups) - 1
        sems = ref["s_send"].at[n, g], ref["s_recv"].at[n, g]
        return buf.at.__getitem__, *sems, lambda k: buf.at[pl.ds(0, k)], direct

    def choose(n, g):
        start, stop = groups[g]
        top = start * tile_slots
        half_count = counted(g)[0]
        count = (stop - start) * width
        columns = slice(start * width, stop * width)
        which = n // chunks
        chunk = min(n, first) * height
        near = ref["pick"][which, top : top + half_count, :count]
        far = ref["pick"][which, top + half_count : top + 2 * half_count, :count]
        high = ref["y_h"][chunk : chunk + height, columns]
        low = ref["y_l"][chunk : chunk + height, columns]
        none = jnp.zeros_like(high)
        chosen = (
            dd(near, jnp.concatenate([high, none], axis=0), 1, 1)
            + dd(near, jnp.concatenate([low, none], axis=0), 1, 1)
            + dd(far, jnp.concatenate([none, high], axis=0), 1, 1)
            + dd(far, jnp.concatenate([none, low], axis=0), 1, 1)
        )
        ref[f"s{n}{g}"][pl.ds(c, 1)] = chosen[None]
        spread(*s_at(n, g))

    done = set()

    def finish(s):
        k, g = stages[s]
        start, stop = groups[g]
        fin = ref[f"f{s}"]
        remote(fin, fin, ref["r_send"].at[s], ref["r_recv"].at[s, 3], mate).wait_recv()
        out = ref[f"t{s}"]
        for base, one, two in ((0, 0, 3), (half, 1, 2)):

            def body(i, base=base, one=one, two=two):
                at = pl.ds(pl.multiple_of(i + base, 8), 8)
                out[0, at, :] = out[0, at, :] + (fin[one, pl.ds(i, 8), :] + fin[two, pl.ds(i, 8), :])

            strips(half, body)
        count = (stop - start) * width
        span = slice(start * width, stop * width)
        high, low = halves_of(out[0, :, :count])
        ref["y_h"][k * height : (k + 1) * height, span] = high
        ref["y_l"][k * height : (k + 1) * height, span] = low
        into, at, target = ("o_one", k, "out_one") if k < first else ("o_two", 0, "out_two")
        for j in range(start, stop):
            ref[into][at, j] = -out[0, :, (j - start) * width : (j + 1 - start) * width]
        write(ref[into].at[at, start:stop], ref[target].at[at, start:stop])
        done.add(s)
        choose(k, g)

    def order(at, owner, slot, g, keep_if):
        start, stop = groups[g]
        half_count, region = counted(g)
        inside = slot - start * tile_slots
        side = (inside >= half_count).astype(jnp.int32)
        mark = side * region + owner * half_count + inside - side * half_count
        mark = jnp.where((inside >= 0) & (inside < 2 * half_count) & keep_if, mark, -1)
        take = ones_at(iota((2 * region, entries), 0) == mark)
        span = slice(0, fringe) if at == 1 else slice(fringe, fringe + width)
        for part, name in (("ph", "h"), ("pl", "l")):
            ref[f"c{at}{g}{name}"][...] = dd(take, ref[part][:, span]).astype(BF16)

    def order_one(g):
        order(1, c_owner1, c_slot1, g, c_owner1 >= 0)

    def order_two(g):
        order(2, c_owner2, c_slot2, g, above)

    def order_low():
        place = (over(row2, TILE) - tiles) * width + within(row2, width)
        mark = jnp.where(above, -1, c_owner2 * fringe + place)
        take = ones_at(iota((cols * fringe, entries), 0) == mark)
        ref["cl_h"][...] = dd(take, ref["ph"][:, fringe:]).astype(BF16)
        ref["cl_l"][...] = dd(take, ref["pl"][:, fringe:]).astype(BF16)

    asides = {0: [lambda: forward(*v_at(first))]}
    for index, work in enumerate(
        [lambda g=g: order_one(g) for g in range(len(groups))]
        + [lambda g=g: order_two(g) for g in range(len(groups))]
        + [order_low]
    ):
        asides.setdefault(1 + index // 2, []).append(work)
    pending = []
    begun = set()

    def settle(s, now):
        if s not in done:
            finish(s)
            pending.append((now + 2, stages[s]))

    def relay(now):
        while pending and pending[0][0] <= now:
            forward(*s_at(*pending.pop(0)[1]))

    gap = 4
    count = len(stages)
    for step in range(count):
        if step >= gap:
            settle(step - gap, step)
        k, g = stages[step]
        if k not in begun:
            begun.add(k)
            ready(k)
        if k >= first:
            for other in range(first):
                settle(names_of[other, g], step)
        begin(step)
        for work in asides.pop(step, []):
            work()
        if step >= 2:
            middle(step - 2)
        push(step)
        relay(step)
    for works in asides.values():
        for work in works:
            work()
    middle(count - 2)
    relay(count)

    def own_rows_of(g):
        choose(chunks, g)
        pending.append((count + 2, (chunks, g)))

    for index in range(len(groups)):
        settle(count - len(groups) + index, count)
        own_rows_of(index)
        if index == 0:
            middle(count - 1)
        else:
            relay(count + 2)
    relay(count + 2)

    def side_by_side(n, g):
        region = counted(g)[1]
        buf = ref[f"s{n}{g}"]
        return halves_of(grown(jnp.concatenate([buf[q] for q in range(cols)], axis=0), region).T)

    def ordered(at, g, side):
        region = counted(g)[1]
        span = slice(side * region, (side + 1) * region)
        return ref[f"c{at}{g}h"][span], ref[f"c{at}{g}l"][span]

    def crossed(n, g, at):
        arrive(*s_at(n, g))
        both = side_by_side(n, g)
        near = three(both, ordered(at, g, 0))[:height]
        return near + three(both, ordered(at, g, 1))[height:]

    cross = jnp.zeros((height, fringe), F32)
    for g in range(len(groups)):
        cross = cross + crossed(first, g, 1)
    tail = ref[f"t{len(stages) - 1}"]
    bottom = cross - tail[0, :, tail.shape[2] - fringe :]
    ref["b"][pl.ds(c, 1)] = bottom[None]
    for step in range(1, cols):
        other = (c + step) % cols
        launch(
            remote(
                ref["b"].at[c], ref["b"].at[c], ref["b_send"], ref["b_recv"].at[c], r, other
            )
        )
    sent(lambda: ref["b"].at[pl.ds(0, cols - 1)], ref["b_send"])
    for kk in range(first):
        ref["o_two"][0, tiles + kk] = bottom[:, kk * width : (kk + 1) * width]
    for k in range(first):
        corner = jnp.zeros((height, fringe), F32)
        for g in range(len(groups)):
            corner = corner + crossed(k, g, 1)
        for kk in range(first):
            piece = corner[:, kk * width : (kk + 1) * width]
            ref["o_one"][k, tiles + kk] = ref["d_one"][k, kk] + piece
        write(ref["o_one"].at[k, tiles:], ref["out_one"].at[k, tiles:])
    result = ref["d_two"][0, 0]
    for g in range(len(groups)):
        result = result + crossed(chunks, g, 2)
    for step in range(1, cols):
        other = (c + step) % cols
        remote(
            ref["b"].at[other], ref["b"].at[other], ref["b_send"], ref["b_recv"].at[other], r, other
        ).wait_recv()
    for q in range(cols):
        span = slice(q * fringe, (q + 1) * fringe)
        result = result - three(halves_of(ref["b"][q]), (ref["cl_h"][span], ref["cl_l"][span]))
    ref["o_two"][0, tiles + first] = result
    write(ref["o_two"].at[0, tiles:], ref["out_two"].at[0, tiles:])

    for go, wait in ends:
        if go is None:
            wait()
        else:
            pl.when(go)(wait)
    for copy in writes:
        copy.wait()


def leave(one, two, out_one, out_two, held_one, held_two, sems):
    pieces = [(one, held_one, out_one, k) for k in range(one.shape[0])] + [(two, held_two, out_two, 0)]

    def copy(source, target, k, index):
        return pltpu.make_async_copy(source.at[k], target.at[k], sems.at[index])

    ins = [copy(a, b, k, n) for n, (a, b, _, k) in enumerate(pieces)]
    outs = [copy(b, a, k, n + len(pieces)) for n, (_, b, a, k) in enumerate(pieces)]
    for each in ins:
        each.start()
    for taken, given in zip(ins, outs):
        taken.wait()
        given.start()
    for each in outs:
        each.wait()


def on_device_fused(
    ancestor,
    inverse_first,
    panel_first,
    structure_first,
    inverse_second,
    panel_second,
    structure_second,
):
    rows = lax.axis_size("row")
    cols = lax.axis_size("col")
    height = TILE // rows
    width = TILE // cols
    tiles = ancestor.shape[0]
    first = inverse_first.shape[0]
    entries = structure_first.shape[0]
    chunks = first + 1
    wide = tiles * width
    row_slots = tiles * height // GRAIN * CAP
    low_slots = first * height // GRAIN * CAP
    col_slots = wide // GRAIN * CAP
    row_pad = -(-row_slots // 128) * 128
    edge = first * height
    fringe = first * width
    parts = min(3, tiles)
    counts = [tiles // parts + (i < tiles % parts) for i in range(parts)]
    if counts[-1] > 1:
        counts[0] += 1
        counts[-1] -= 1
    groups = [(sum(counts[:i]), sum(counts[: i + 1])) for i in range(parts)]
    widest = max(stop - start for start, stop in groups) * width
    stages = chunks * parts
    dma = pltpu.SemaphoreType.DMA
    scratch = {
        "a": pltpu.VMEM((tiles, tiles, height, width), F32),
        "d_one": pltpu.VMEM((first, first, height, width), F32),
        "d_two": pltpu.VMEM((1, 1, height, width), F32),
        "l_one": pltpu.VMEM((entries,), jnp.int32),
        "l_two": pltpu.VMEM((entries,), jnp.int32),
        "o_one": pltpu.VMEM((first, tiles + first, height, width), F32),
        "o_two": pltpu.VMEM((1, tiles + first + 1, height, width), F32),
        "own": pltpu.VMEM((chunks, entries // rows, width), F32),
        "pall": pltpu.VMEM((chunks, entries, width), F32),
        "ph": pltpu.VMEM((entries, chunks * width), BF16),
        "pl": pltpu.VMEM((entries, chunks * width), BF16),
        "kept_h": pltpu.VMEM((2, row_pad, wide), BF16),
        "kept_l": pltpu.VMEM((2, row_pad, wide), BF16),
        "v_one": pltpu.VMEM((first, cols, row_slots, width), F32),
        "v_two": pltpu.VMEM((cols, row_slots + low_slots, width), F32),
        "turned": pltpu.VMEM((chunks, 8 * width, row_pad), BF16),
        "under": pltpu.VMEM((8 * width, edge), BF16),
        "y_h": pltpu.VMEM((chunks * height, wide), BF16),
        "y_l": pltpu.VMEM((chunks * height, wide), BF16),
        "d_h": pltpu.VMEM((edge, fringe), BF16),
        "d_l": pltpu.VMEM((edge, fringe), BF16),
        "pick": pltpu.VMEM((2, col_slots, widest), BF16),
        "cl_h": pltpu.VMEM((cols * fringe, width), BF16),
        "cl_l": pltpu.VMEM((cols * fringe, width), BF16),
        "b": pltpu.VMEM((cols, height, fringe), F32),
        "l_sem": dma((5 + chunks,)),
        "w_sem": dma((stages + first + 1,)),
        "g_send": dma((chunks,)),
        "g_recv": dma((chunks, 4)),
        "v_send": dma((chunks,)),
        "v_recv": dma((chunks, cols)),
        "r_send": dma((stages,)),
        "r_recv": dma((stages, 4)),
        "s_send": dma((chunks + 1, parts)),
        "s_recv": dma((chunks + 1, parts, cols)),
        "b_send": dma,
        "b_recv": dma((cols,)),
    }
    for g, (start, stop) in enumerate(groups):
        count = (stop - start) * width // GRAIN * CAP // 2
        region = -(-count * cols // 128) * 128
        for n in range(chunks + 1):
            scratch[f"s{n}{g}"] = pltpu.VMEM((cols, count, 2 * height), F32)
        for name in ("h", "l"):
            scratch[f"c1{g}{name}"] = pltpu.VMEM((2 * region, fringe), BF16)
            scratch[f"c2{g}{name}"] = pltpu.VMEM((2 * region, width), BF16)
    for s, (k, g) in enumerate(order_of(first, parts)):
        size = (groups[g][1] - groups[g][0]) * width
        if s == stages - 1:
            size += fringe
        scratch[f"z{s}"] = pltpu.VMEM((8, height, size), F32)
        scratch[f"m{s}"] = pltpu.VMEM((4, height, size), F32)
        scratch[f"t{s}"] = pltpu.VMEM((4, height, size), F32)
        scratch[f"i{s}"] = pltpu.VMEM((2, height // 2, size), F32)
        scratch[f"f{s}"] = pltpu.VMEM((4, height // 2, size), F32)
    inputs = ["ancestor", "diag_one", "diag_two", "panel_one", "panel_two", "list_one", "list_two"]
    names = inputs + ["out_one", "out_two"] + list(scratch)
    hbm = pl.BlockSpec(memory_space=pl.ANY)
    dims = (rows, cols, height, width, tiles, first, entries, groups)
    shapes = (
        jax.ShapeDtypeStruct((first, tiles + first, height, width), F32),
        jax.ShapeDtypeStruct((1, tiles + first + 1, height, width), F32),
    )
    results = pl.pallas_call(
        functools.partial(fused, dims, names),
        out_shape=shapes,
        in_specs=[hbm] * len(inputs),
        out_specs=(hbm, hbm),
        scratch_shapes=list(scratch.values()),
        compiler_params=pltpu.CompilerParams(
            collective_id=0, has_side_effects=True, vmem_limit_bytes=60 * 1024 * 1024
        ),
    )(
        open_packed(ancestor, height, width),
        open_packed(inverse_first, height, width),
        open_packed(inverse_second, height, width),
        panel_first,
        panel_second,
        structure_first,
        structure_second,
    )
    return pl.pallas_call(
        leave,
        out_shape=shapes,
        in_specs=[hbm, hbm],
        out_specs=(hbm, hbm),
        scratch_shapes=[
            pltpu.VMEM(shapes[0].shape, F32),
            pltpu.VMEM(shapes[1].shape, F32),
            dma((2 * (first + 1),)),
        ],
        compiler_params=pltpu.CompilerParams(vmem_limit_bytes=60 * 1024 * 1024),
    )(*results)


def fits(rows, cols):
    return rows == 8 and rows == 2 * cols and TILE // cols % 128 == 0


def solution(mesh):
    body = on_device_fused if fits(mesh.shape["row"], mesh.shape["col"]) else on_device
    in_specs = (
        P(None, None, "row", "col"),
        P(None, None, "row", "col"),
        P("row", None, "col"),
        P(),
        P(None, None, "row", "col"),
        P("row", None, "col"),
        P(),
    )
    out_specs = (P(None, None, "row", "col"), P(None, None, "row", "col"))
    return jax.shard_map(
        body, mesh=mesh, in_specs=in_specs, out_specs=out_specs, check_vma=False
    )
```

```python
import functools

import jax
import jax.numpy as jnp
from jax import lax
from jax.experimental import pallas as pl
from jax.experimental.pallas import tpu as pltpu
from jax.sharding import PartitionSpec as P

TILE = 512
GRAIN = 16
CAP = 6


def open_packed(packed, row_height, col_width):
    return packed.reshape(packed.shape[0], packed.shape[1], row_height, col_width)


def close_packed(tiles):
    depth = tiles.shape[2] * tiles.shape[3] // 128
    return tiles.reshape(tiles.shape[0], tiles.shape[1], depth, 128)


def product(left, right, left_dim=1):
    return lax.dot_general(
        left,
        right,
        (((left_dim,), (0,)), ((), ())),
        precision=lax.Precision.HIGH,
        preferred_element_type=jnp.float32,
    )


def entry_ranks(structure):
    group = structure // GRAIN
    order = jnp.arange(structure.shape[0], dtype=jnp.int32)
    same = (group[:, None] == group[None, :]) & (order[None, :] < order[:, None])
    return jnp.sum(same.astype(jnp.int32), axis=1)


def slots_within(structure, ranks, height):
    owner = structure % TILE // height
    group = structure // TILE * (height // GRAIN) + structure % height // GRAIN
    return owner, group * CAP + ranks


def one_hot(marks, count):
    return (jnp.arange(count, dtype=jnp.int32)[:, None] == marks[None, :]).astype(jnp.float32)


def local_rows(structure, marks, count, height):
    row = structure // TILE * height + structure % height
    match = jnp.arange(count, dtype=jnp.int32)[:, None] == marks[None, :]
    return jnp.max(jnp.where(match, row[None, :], -1), axis=1)


def on_device(
    ancestor,
    inverse_first,
    panel_first,
    structure_first,
    inverse_second,
    panel_second,
    structure_second,
):
    rows = lax.axis_size("row")
    cols = lax.axis_size("col")
    height = TILE // rows
    width = TILE // cols
    halves = width // height
    row_index = lax.axis_index("row")
    col_index = lax.axis_index("col")
    blocks = open_packed(ancestor, height, width)
    first_diag = open_packed(inverse_first, height, width)
    second_diag = open_packed(inverse_second, height, width)
    tiles = blocks.shape[0]
    first = first_diag.shape[0]
    second = second_diag.shape[0]
    every = first + second
    limit = tiles * TILE
    first_width = first * width

    panels = jnp.concatenate(
        [panel_first.reshape(-1, first_width), panel_second.reshape(-1, second * width)], axis=1
    )
    both = lax.all_gather(panels, "row", axis=0, tiled=True)
    whole_first = both[:, :first_width]
    whole_second = both[:, first_width:]

    above = structure_second < limit
    ranks_first = entry_ranks(structure_first)
    ranks_second = entry_ranks(structure_second)
    row_slots = tiles * height // GRAIN * CAP
    col_slots = tiles * width // GRAIN * CAP
    low_slots = first * TILE // GRAIN * CAP
    owner, slot = slots_within(structure_first, ranks_first, height)
    row_marks_first = jnp.where(owner == row_index, slot, -1)
    owner, slot = slots_within(structure_second, ranks_second, height)
    row_marks_second = jnp.where(above & (owner == row_index), slot, -1)
    owner, slot = slots_within(structure_first, ranks_first, width)
    all_marks_first = owner * col_slots + slot
    col_marks_first = jnp.where(owner == col_index, slot, -1)
    owner, slot = slots_within(structure_second, ranks_second, width)
    all_marks_second = jnp.where(above, owner * col_slots + slot, -1)
    col_marks_second = jnp.where(above & (owner == col_index), slot, -1)
    below = structure_second - limit
    low_marks = jnp.where(above, -1, below // GRAIN * CAP + ranks_second)
    low_match = jnp.arange(low_slots, dtype=jnp.int32)[:, None] == low_marks[None, :]
    low_rows = jnp.max(jnp.where(low_match, below[None, :], -1), axis=1)

    take_first = one_hot(row_marks_first, row_slots)
    take_second = one_hot(
        jnp.where(above, row_marks_second, row_slots + low_marks), row_slots + low_slots
    )
    part_first = product(take_first, whole_first)
    part_second = product(take_second, whole_second)
    part_first = part_first.reshape(row_slots, first, halves, height).transpose(0, 2, 1, 3)
    part_first = part_first.reshape(row_slots * first, width)
    part_second = part_second.reshape(row_slots + low_slots, second, halves, height)
    part_second = part_second.transpose(0, 2, 1, 3)
    part_second = part_second.reshape((row_slots + low_slots) * second, width)
    spread = lax.all_gather(jnp.concatenate([part_first, part_second], axis=0), "col", axis=0)
    cut = part_first.shape[0]
    got_first = spread[:, :cut].reshape(cols, row_slots, halves, first, height)
    got_second = spread[:, cut:].reshape(cols, row_slots + low_slots, halves, second, height)
    got_first = got_first.transpose(1, 0, 2, 3, 4).reshape(row_slots, rows, first * height)
    got_second = got_second.transpose(1, 0, 2, 3, 4).reshape(-1, rows, second * height)
    upper_second = got_second[:row_slots]
    low_second = got_second[row_slots:].reshape(low_slots, second * TILE)

    flat = blocks.transpose(0, 2, 1, 3).reshape(tiles * height, tiles * width)
    kept_rows = jnp.concatenate(
        [
            local_rows(structure_first, row_marks_first, row_slots, height),
            local_rows(structure_second, row_marks_second, row_slots, height),
        ]
    )
    take_kept = (
        kept_rows[:, None] == jnp.arange(tiles * height, dtype=jnp.int32)[None, :]
    ).astype(jnp.float32)
    kept = product(take_kept, flat)

    place = jnp.arange(first * TILE, dtype=jnp.int32)
    place_row = place // (first * height)
    place_tile = place // height % first
    named = place_tile * TILE + place_row * height + place % height
    meet_low = (named[:, None] == low_rows[None, :]).astype(jnp.float32)
    first_at_low = product(got_first.reshape(row_slots, first * TILE), meet_low)
    folded = product(first_at_low, low_second).reshape(row_slots, rows, second * height)
    left = jnp.concatenate(
        [
            jnp.concatenate([got_first, -folded], axis=2),
            jnp.concatenate(
                [jnp.zeros((row_slots, rows, first * height), jnp.float32), upper_second], axis=2
            ),
        ],
        axis=0,
    )
    partial = product(left.reshape(2 * row_slots, every * TILE), kept, 0)
    partial = partial.reshape(rows, every * height, tiles * width)

    own_low = jnp.arange(first * height, dtype=jnp.int32)
    own_low = own_low // height * TILE + row_index * height + own_low % height
    own_meet = (own_low[:, None] == low_rows[None, :]).astype(jnp.float32)
    own_second = product(own_meet, low_second)
    flat_diag = first_diag.transpose(0, 2, 1, 3).reshape(first * height, first_width)
    low_partial = product(own_second, flat_diag, 0)
    low_partial = low_partial.reshape(rows, second * height, first_width)

    slabs = [low_partial[:, :, k * width : (k + 1) * width] for k in range(first)]
    slabs.append(jnp.zeros((rows, (every - first * second) * height, width), jnp.float32))
    joined = jnp.concatenate([partial, jnp.concatenate(slabs, axis=1)], axis=2)
    summed = lax.psum_scatter(joined, "row", scatter_dimension=0, tiled=False)
    image = summed[:, : tiles * width]
    step = second * height
    low_image = jnp.concatenate(
        [summed[k * step : (k + 1) * step, tiles * width :] for k in range(first)], axis=1
    )

    edge = first * height
    column_ids = jnp.arange(tiles * width, dtype=jnp.int32)
    col_rows_first = local_rows(structure_first, col_marks_first, col_slots, width)
    col_rows_second = local_rows(structure_second, col_marks_second, col_slots, width)
    pick_first = (column_ids[:, None] == col_rows_first[None, :]).astype(jnp.float32)
    pick_second = (column_ids[:, None] == col_rows_second[None, :]).astype(jnp.float32)
    picked = jnp.concatenate([product(image, pick_first), product(image[edge:], pick_second)], axis=0)
    met = lax.all_gather(picked, "col", axis=0)
    met = met.transpose(1, 0, 2).reshape(-1, cols * col_slots)
    dense_first = product(one_hot(all_marks_first, cols * col_slots), whole_first)
    dense_second = product(one_hot(all_marks_second, cols * col_slots), whole_second)
    corner = product(met[: every * height], dense_first)
    low_block = low_image - corner[edge:]
    low_all = lax.all_gather(low_block, "col", axis=0)
    low_all = low_all.transpose(1, 0, 2).reshape(second * height, first * TILE)
    spot = jnp.arange(first * TILE, dtype=jnp.int32)
    spot = spot // width % first * TILE + spot // first_width * width + spot % width
    below_marks = jnp.where(above, -1, below)
    dense_low = product(
        (spot[:, None] == below_marks[None, :]).astype(jnp.float32), whole_second
    )
    final = product(met[every * height :], dense_second) + product(low_all, dense_low)

    def tiled(matrix, up, across):
        return matrix.reshape(up, height, across, width).transpose(0, 2, 1, 3)

    row_first = jnp.concatenate(
        [-tiled(image[:edge], first, tiles), first_diag + tiled(corner[:edge], first, first)], axis=1
    )
    row_second = jnp.concatenate(
        [
            -tiled(image[edge:], second, tiles),
            -tiled(low_block, second, first),
            second_diag + tiled(final, second, second),
        ],
        axis=1,
    )
    return (close_packed(row_first), close_packed(row_second))

F32 = jnp.float32
BF16 = jnp.bfloat16
MESH = pl.DeviceIdType.MESH


def over(value, size):
    return lax.shift_right_logical(value, jnp.int32(size.bit_length() - 1))


def within(value, size):
    return value & jnp.int32(size - 1)


def iota(shape, dim):
    return lax.broadcasted_iota(jnp.int32, shape, dim)


def ones_at(mask):
    return jnp.where(mask, 1.0, 0.0).astype(BF16)


def dd(left, right, left_dim=1, right_dim=0):
    return lax.dot_general(
        left, right, (((left_dim,), (right_dim,)), ((), ())), preferred_element_type=F32
    )


def halves_of(value):
    high = value.astype(BF16)
    return high, (value - high.astype(F32)).astype(BF16)


def three(left, right):
    return dd(left[0], right[0]) + dd(left[0], right[1]) + dd(left[1], right[0])


def grown(value, count):
    rest = count - value.shape[0]
    if not rest:
        return value
    return jnp.concatenate([value, jnp.zeros((rest, value.shape[1]), value.dtype)], axis=0)


def spots(hits, places):
    return jnp.max(jnp.where(hits, places, -1.0), axis=1, keepdims=True)


def order_of(first, parts):
    return [(k, g) for k in range(first + 1) for g in range(parts)]


def fused(dims, names, *refs):
    ref = dict(zip(names, refs))
    rows, cols, height, width, tiles, first, entries, groups = dims
    chunks = first + 1
    shard = entries // rows
    wide = tiles * width
    tall = tiles * height
    row_slots = tall // GRAIN * CAP
    low_slots = first * height // GRAIN * CAP
    tile_slots = width // GRAIN * CAP
    col_slots = tiles * tile_slots
    edge = first * height
    fringe = first * width
    row_pad = -(-row_slots // 128) * 128
    half = height // 2

    r = lax.axis_index("row")
    c = lax.axis_index("col")
    core = r % 2
    chip = r // 2
    chip_x = chip % 2
    chip_y = chip // 2
    by_x = r + 2 - 4 * chip_x
    by_y = r + 4 - 8 * chip_y
    by_both = r + 6 - 4 * chip_x - 8 * chip_y
    mate = r + 1 - 2 * core
    peers = {1: by_x, 2: by_y, 3: by_both}

    def chip_at(rel):
        x = 1 - chip_x if rel % 2 else chip_x
        y = 1 - chip_y if rel // 2 else chip_y
        return y * 2 + x

    ends = []

    def remote(source, target, send, recv, device, column=None):
        return pltpu.make_async_remote_copy(
            src_ref=source,
            dst_ref=target,
            send_sem=send,
            recv_sem=recv,
            device_id=(device, c if column is None else column),
            device_id_type=MESH,
        )

    def launch(copy):
        copy.start()
        return copy

    def sent(whole, sem, go=None):
        ends.append((go, lambda: remote(whole(), whole(), sem, sem, mate).wait_send()))

    barrier = pltpu.get_barrier_semaphore()
    for peer in (mate, by_x, by_y, by_both):
        pl.semaphore_signal(barrier, inc=1, device_id=(peer, c), device_id_type=MESH)
    for step in range(1, cols):
        other = (c + step) % cols
        pl.semaphore_signal(barrier, inc=1, device_id=(r, other), device_id_type=MESH)
    loads = {}

    def load(name, source, target):
        loads[name] = pltpu.make_async_copy(source, target, ref["l_sem"].at[len(loads)])
        loads[name].start()

    load("list_one", ref["list_one"], ref["l_one"])
    load("list_two", ref["list_two"], ref["l_two"])
    for k in range(chunks):
        source = ref["panel_one"].at[:, k] if k < first else ref["panel_two"].at[:, k - first]
        load(k, source, ref["own"].at[k])
    load("a", ref["ancestor"], ref["a"])
    load("d_one", ref["diag_one"], ref["d_one"])
    load("d_two", ref["diag_two"], ref["d_two"])

    def ranks(row):
        group = over(row, GRAIN)
        total = [jnp.zeros((1, 128), F32) for _ in range(entries // 128)]
        lanes = iota((128, 128), 1)
        order = iota((128, 128), 0)
        for b in range(entries // 128):
            one = group[:, b * 128 : (b + 1) * 128]
            column = jnp.broadcast_to(one, (128, 128)).T
            for t in range(b, entries // 128):
                hit = column == group[:, t * 128 : (t + 1) * 128]
                if t == b:
                    hit = hit & (order < lanes)
                total[t] = total[t] + jnp.sum(jnp.where(hit, 1.0, 0.0), axis=0, keepdims=True)
        return jnp.concatenate(total, axis=1).astype(jnp.int32)

    def owned(row, rank, size):
        owner = over(within(row, TILE), size)
        group = over(row, TILE) * (size // GRAIN) + over(within(row, size), GRAIN)
        place = over(row, TILE) * size + within(row, size)
        return owner, group * CAP + rank, place.astype(F32)

    loads["list_one"].wait()
    loads["list_two"].wait()
    row1 = ref["l_one"][...].reshape(1, entries)
    row2 = ref["l_two"][...].reshape(1, entries)
    rank1 = ranks(row1)
    rank2 = ranks(row2)
    above = row2 < tiles * TILE
    r_owner1, r_slot1, r_place1 = owned(row1, rank1, height)
    r_owner2, r_slot2, r_place2 = owned(row2, rank2, height)
    c_owner1, c_slot1, c_place1 = owned(row1, rank1, width)
    c_owner2, c_slot2, c_place2 = owned(row2, rank2, width)
    mark1 = jnp.where(r_owner1 == r, r_slot1, -1)
    mark2 = jnp.where(r_owner2 == r, r_slot2, -1)
    upper2 = jnp.where(above, mark2, -1)
    lower2 = jnp.where(above | (r_owner2 != r), -1, r_slot2 - row_slots)

    pl.semaphore_wait(barrier, 4 + cols - 1)
    pall = ref["pall"]

    def own_rows(device):
        return pl.ds(pl.multiple_of(device * shard, 8), shard)

    gather = {}
    for k in range(chunks):
        loads[k].wait()
        for rel, peer in (*peers.items(), (0, mate)):
            gather[k, rel] = launch(
                remote(
                    ref["own"].at[k],
                    pall.at[k, own_rows(r)],
                    ref["g_send"].at[k],
                    ref["g_recv"].at[k, rel],
                    peer,
                )
            )
        sent(lambda k=k: pall.at[k, pl.ds(0, 7 * shard)], ref["g_send"].at[k])
    for k in range(chunks):
        pall[k, own_rows(r), :] = ref["own"][k]

    def keep(at, marks, places):
        spot = spots(iota((row_pad, entries), 0) == marks, places)
        take = ones_at(spot == iota((row_pad, tall), 1).astype(F32))

        def step(j, carry):
            block = ref["a"][:, pl.ds(j, 1), :, :].reshape(tall, width)
            high, low = halves_of(block)
            span = pl.ds(pl.multiple_of(j * width, 128), width)
            ref["kept_h"][at, :, span] = dd(take, high).astype(BF16)
            ref["kept_l"][at, :, span] = dd(take, low).astype(BF16)
            return carry

        lax.fori_loop(0, tiles, step, 0)

    def spread(at, sends, recvs, whole, direct=False):
        for sign, reach in ((1, 3), (-1, 3), (1, 2), (-1, 2), (1, 1), (-1, 1)):
            there = c + sign * reach
            if reach < cols - 1 or direct:

                @pl.when((there >= 0) & (there < cols))
                def _(there=there):
                    remote(at(c), at(c), sends, recvs.at[c], r, there).start()

        if direct:
            sent(lambda: whole(cols - 1), sends)
        else:
            edge_of = (c == 0) | (c == cols - 1)
            sent(lambda: whole(2), sends, edge_of)
            sent(lambda: whole(4), sends, jnp.logical_not(edge_of))

    def forward(at, sends, recvs, whole, direct=False):
        if direct:
            return
        for sign in (1, -1):
            q = c - 2 * sign
            there = c + sign

            @pl.when((q >= 0) & (q < cols) & (there >= 0) & (there < cols))
            def _(q=q, there=there):
                copy = remote(at(q), at(q), sends, recvs.at[q], r, there)
                copy.wait_recv()
                copy.start()

    def arrive(at, sends, recvs, whole, direct=False):
        for reach in range(1, cols):
            for sign in (1, -1):
                q = c - reach * sign
                there = c + sign
                go = (q >= 0) & (q < cols)
                if reach == 2 and not direct:
                    go = go & ((there < 0) | (there >= cols))

                @pl.when(go)
                def _(q=q):
                    remote(at(q), at(q), sends, recvs.at[q], r, c).wait_recv()

    def v_at(k):
        buf = ref["v_one"].at[k] if k < first else ref["v_two"]
        return buf.at.__getitem__, ref["v_send"].at[k], ref["v_recv"].at[k], lambda n: buf.at[pl.ds(0, n)]

    one_rows = -(-row_slots // 16) * 16
    two_rows = -(-(row_slots + low_slots) // 16) * 16
    take1 = ones_at(iota((one_rows, entries), 0) == mark1)
    loads["a"].wait()
    keep(0, mark1, r_place1)
    for k in range(chunks):
        for rel in (1, 2, 3):
            gather[k, rel].wait_recv()
            part = pall.at[k, own_rows(peers[rel])]
            gather[k, 3 + rel] = launch(
                remote(part, part, ref["g_send"].at[k], ref["g_recv"].at[k, 0], mate)
            )
        four = pall.at[k, pl.ds(0, 4 * shard)]
        remote(four, four, ref["g_send"].at[k], ref["g_recv"].at[k, 0], mate).wait_recv()
        high, low = halves_of(pall[k])
        span = slice(k * width, (k + 1) * width)
        ref["ph"][:, span] = high
        ref["pl"][:, span] = low
        take = take1 if k < first else ones_at(iota((two_rows, entries), 0) == mark2)
        picked = dd(take, high) + dd(take, low)
        if k < first:
            ref["v_one"][k, pl.ds(c, 1)] = picked[None, :row_slots]
        else:
            ref["v_two"][pl.ds(c, 1)] = picked[None, : row_slots + low_slots]
        if k:
            forward(*v_at(k - 1))
        spread(*v_at(k))

    low_spot = spots(iota((128, entries), 0) == lower2, r_place2 - float(tall))
    spread_low = ones_at(low_spot == iota((128, edge), 1).astype(F32))
    loads["d_one"].wait()
    loads["d_two"].wait()
    for k in range(first):
        for kk in range(first):
            high, low = halves_of(ref["d_one"][k, kk])
            ref["d_h"][k * height : (k + 1) * height, kk * width : (kk + 1) * width] = high
            ref["d_l"][k * height : (k + 1) * height, kk * width : (kk + 1) * width] = low

    def picker(which, owner, slot, place, extra=None):
        mine = owner == c
        if extra is not None:
            mine = mine & extra
        spot = spots(iota((col_slots, entries), 0) == jnp.where(mine, slot, -1), place)
        for start, stop in groups:
            span = slice(start * tile_slots, stop * tile_slots)
            count = (stop - start) * width
            here = iota(((stop - start) * tile_slots, count), 1) + start * width
            ref["pick"][which, span, :count] = ones_at(spot[span] == here.astype(F32))

    def ready(k):
        arrive(*v_at(k))
        for rel in range(4):
            klass = chip_at(rel)
            if k < first:
                value = ref["v_one"][k, pl.ds(klass, 1)].reshape(row_slots, width)
            else:
                both = ref["v_two"][pl.ds(klass, 1)].reshape(row_slots + low_slots, width)
                value = both[:row_slots]
                under = halves_of(grown(both[row_slots:], 128).T)
                under = halves_of(dd(under[0], spread_low) + dd(under[1], spread_low))
                for n in range(2):
                    start = (4 * n + rel) * width
                    ref["under"][start : start + width, :] = under[n]
            turned = halves_of(grown(value, row_pad).T)
            for n in range(2):
                start = (4 * n + rel) * width
                ref["turned"][k, start : start + width, :] = turned[n]

    def stacked(left, high, low):
        count = left.shape[0] // 2
        both = dd(left, high)
        return both[:count] + both[count:] + dd(left[:count], low)

    stages = order_of(first, len(groups))
    names_of = {stage: s for s, stage in enumerate(stages)}
    live = {}

    def put(s, part, start, stop):
        for rel in range(4):
            for side in range(2):
                top = rel * width + side * height
                ref[f"z{s}"][side * 4 + rel, :, start:stop] = part[top : top + height]

    def begin(s):
        k, g = stages[s]
        start, stop = groups[g]
        span = slice(start * width, stop * width)
        count = (stop - start) * width
        at = 0 if k < first else 1
        part = stacked(ref["turned"][k], ref["kept_h"][at, :, span], ref["kept_l"][at, :, span])
        if k >= first:
            part = part - stacked(ref["under"][...], ref["y_h"][:edge, span], ref["y_l"][:edge, span])
        put(s, part, 0, count)
        if k >= first and g == len(groups) - 1:
            part = stacked(ref["under"][...], ref["d_h"][...], ref["d_l"][...])
            put(s, part, count, count + fringe)
        live[s, 0] = launch(
            remote(
                ref[f"z{s}"].at[pl.ds((1 - core) * 4, 4)],
                ref[f"m{s}"],
                ref["r_send"].at[s],
                ref["r_recv"].at[s, 0],
                mate,
            )
        )
        sent(lambda: ref[f"z{s}"].at[pl.ds(0, 7)], ref["r_send"].at[s])

    def strips(count, body):
        def step(i, carry):
            body(pl.multiple_of(i * 8, 8))
            return carry

        lax.fori_loop(0, count // 8, step, 0)

    def pass_on(s, index, source, target, peer):
        live[s, index] = launch(
            remote(source, target, ref["r_send"].at[s], ref["r_recv"].at[s, min(index, 3)], peer)
        )

    lower = pl.ds(0, half)
    upper = pl.ds(half, half)

    def push(s):
        live[s, 0].wait_recv()
        total = ref[f"t{s}"]
        got = ref[f"m{s}"]
        own = ref[f"z{s}"]
        count = total.shape[2]

        def pair(rel):
            def body(i):
                at = pl.ds(i, 8)
                mine = own[pl.ds(core * 4 + rel, 1), at, :].reshape(8, count)
                total[rel, at, :] = mine + got[rel, at, :]

            strips(height, body)

        pair(3)
        pass_on(s, 1, total.at[3, lower], ref[f"i{s}"].at[0], by_x)
        pass_on(s, 2, total.at[3, upper], ref[f"i{s}"].at[1], by_y)
        pair(1)
        pass_on(s, 3, total.at[1, lower], ref[f"f{s}"].at[0], by_x)
        pair(2)
        pass_on(s, 4, total.at[2, upper], ref[f"f{s}"].at[1], by_y)
        pair(0)

    summed = set()

    def middle(s):
        if s in summed:
            return
        summed.add(s)
        total = ref[f"t{s}"]
        live[s, 2].wait_recv()

        def body(i):
            at = pl.ds(pl.multiple_of(i + half, 8), 8)
            total[1, at, :] = total[1, at, :] + ref[f"i{s}"][1, pl.ds(i, 8), :]

        strips(half, body)
        pass_on(s, 5, total.at[1, upper], ref[f"f{s}"].at[2], by_x)
        live[s, 1].wait_recv()

        def body(i):
            at = pl.ds(i, 8)
            total[2, at, :] = total[2, at, :] + ref[f"i{s}"][0, at, :]

        strips(half, body)
        pass_on(s, 6, total.at[2, lower], ref[f"f{s}"].at[3], by_y)

    writes = []

    def write(source, target):
        copy = pltpu.make_async_copy(source, target, ref["w_sem"].at[len(writes)])
        copy.start()
        writes.append(copy)

    def counted(g):
        start, stop = groups[g]
        count = (stop - start) * tile_slots // 2
        return count, -(-count * cols // 128) * 128

    def s_at(n, g):
        buf = ref[f"s{n}{g}"]
        direct = n >= first and g == len(groups) - 1
        sems = ref["s_send"].at[n, g], ref["s_recv"].at[n, g]
        return buf.at.__getitem__, *sems, lambda k: buf.at[pl.ds(0, k)], direct

    def choose(n, g):
        start, stop = groups[g]
        top = start * tile_slots
        half_count = counted(g)[0]
        count = (stop - start) * width
        columns = slice(start * width, stop * width)
        which = n // chunks
        chunk = min(n, first) * height
        near = ref["pick"][which, top : top + half_count, :count]
        far = ref["pick"][which, top + half_count : top + 2 * half_count, :count]
        high = ref["y_h"][chunk : chunk + height, columns]
        low = ref["y_l"][chunk : chunk + height, columns]
        none = jnp.zeros_like(high)
        chosen = (
            dd(near, jnp.concatenate([high, none], axis=0), 1, 1)
            + dd(near, jnp.concatenate([low, none], axis=0), 1, 1)
            + dd(far, jnp.concatenate([none, high], axis=0), 1, 1)
            + dd(far, jnp.concatenate([none, low], axis=0), 1, 1)
        )
        ref[f"s{n}{g}"][pl.ds(c, 1)] = chosen[None]
        spread(*s_at(n, g))

    done = set()

    def finish(s):
        k, g = stages[s]
        start, stop = groups[g]
        fin = ref[f"f{s}"]
        remote(fin, fin, ref["r_send"].at[s], ref["r_recv"].at[s, 3], mate).wait_recv()
        out = ref[f"t{s}"]
        for base, one, two in ((0, 0, 3), (half, 1, 2)):

            def body(i, base=base, one=one, two=two):
                at = pl.ds(pl.multiple_of(i + base, 8), 8)
                out[0, at, :] = out[0, at, :] + (fin[one, pl.ds(i, 8), :] + fin[two, pl.ds(i, 8), :])

            strips(half, body)
        count = (stop - start) * width
        span = slice(start * width, stop * width)
        high, low = halves_of(out[0, :, :count])
        ref["y_h"][k * height : (k + 1) * height, span] = high
        ref["y_l"][k * height : (k + 1) * height, span] = low
        into, at, target = ("o_one", k, "out_one") if k < first else ("o_two", 0, "out_two")
        for j in range(start, stop):
            ref[into][at, j] = -out[0, :, (j - start) * width : (j + 1 - start) * width]
        write(ref[into].at[at, start:stop], ref[target].at[at, start:stop])
        done.add(s)
        choose(k, g)

    def order(at, owner, slot, g, keep_if):
        start, stop = groups[g]
        half_count, region = counted(g)
        inside = slot - start * tile_slots
        side = (inside >= half_count).astype(jnp.int32)
        mark = side * region + owner * half_count + inside - side * half_count
        mark = jnp.where((inside >= 0) & (inside < 2 * half_count) & keep_if, mark, -1)
        take = ones_at(iota((2 * region, entries), 0) == mark)
        span = slice(0, fringe) if at == 1 else slice(fringe, fringe + width)
        for part, name in (("ph", "h"), ("pl", "l")):
            ref[f"c{at}{g}{name}"][...] = dd(take, ref[part][:, span]).astype(BF16)

    def order_one(g):
        order(1, c_owner1, c_slot1, g, c_owner1 >= 0)

    def order_two(g):
        order(2, c_owner2, c_slot2, g, above)

    def order_low():
        place = (over(row2, TILE) - tiles) * width + within(row2, width)
        mark = jnp.where(above, -1, c_owner2 * fringe + place)
        take = ones_at(iota((cols * fringe, entries), 0) == mark)
        ref["cl_h"][...] = dd(take, ref["ph"][:, fringe:]).astype(BF16)
        ref["cl_l"][...] = dd(take, ref["pl"][:, fringe:]).astype(BF16)

    asides = {
        1: [lambda: keep(1, upper2, r_place2)],
        2: [
            lambda: forward(*v_at(first)),
            lambda: picker(0, c_owner1, c_slot1, c_place1),
            lambda: picker(1, c_owner2, c_slot2, c_place2, above),
        ],
    }
    for index, g in enumerate(range(len(groups))):
        asides.setdefault(3 + index, []).append(lambda g=g: order_one(g))
    pending = []
    begun = set()

    def settle(s, now):
        if s not in done:
            finish(s)
            if stages[s][0] < first:
                pending.append((now + 2, stages[s]))

    def relay(now):
        while pending and pending[0][0] <= now:
            forward(*s_at(*pending.pop(0)[1]))

    gap = 4
    count = len(stages)
    for step in range(count):
        if step >= gap:
            settle(step - gap, step)
        k, g = stages[step]
        if k not in begun:
            begun.add(k)
            ready(k)
        if k >= first:
            for s in range(first * len(groups)):
                middle(s)
            for other in range(first):
                settle(names_of[other, g], step)
        begin(step)
        for work in asides.pop(step, []):
            work()
        if step >= 2:
            middle(step - 2)
        push(step)
        relay(step)
    middle(count - 2)
    late = len(groups) - 1
    for g in range(len(groups)):
        if g == 1:
            middle(count - 1)
            relay(count + 2)
        finish(stages.index((first, g)))
        if g:
            forward(*s_at(first, g - 1))
    for g in range(len(groups)):
        choose(chunks, g)
    for g in range(late):
        order_two(g)
    forward(*s_at(chunks, 0))
    order_two(late)
    order_low()
    for g in range(1, late):
        forward(*s_at(chunks, g))

    def side_by_side(n, g):
        region = counted(g)[1]
        buf = ref[f"s{n}{g}"]
        return halves_of(grown(jnp.concatenate([buf[q] for q in range(cols)], axis=0), region).T)

    def ordered(at, g, side):
        region = counted(g)[1]
        span = slice(side * region, (side + 1) * region)
        return ref[f"c{at}{g}h"][span], ref[f"c{at}{g}l"][span]

    def crossed(n, g, at):
        arrive(*s_at(n, g))
        both = side_by_side(n, g)
        near = three(both, ordered(at, g, 0))[:height]
        return near + three(both, ordered(at, g, 1))[height:]

    def corner(k):
        total = jnp.zeros((height, fringe), F32)
        for g in range(len(groups)):
            total = total + crossed(k, g, 1)
        for kk in range(first):
            piece = total[:, kk * width : (kk + 1) * width]
            ref["o_one"][k, tiles + kk] = ref["d_one"][k, kk] + piece
        write(ref["o_one"].at[k, tiles:], ref["out_one"].at[k, tiles:])

    tail = ref[f"t{len(stages) - 1}"]
    cross = -tail[0, :, tail.shape[2] - fringe :]
    for g in range(len(groups)):
        cross = cross + crossed(first, g, 1)
    ref["b"][pl.ds(c, 1)] = cross[None]
    b_at = (
        ref["b"].at.__getitem__,
        ref["b_send"],
        ref["b_recv"],
        lambda n: ref["b"].at[pl.ds(0, n)],
    )
    spread(*b_at)
    for kk in range(first):
        ref["o_two"][0, tiles + kk] = cross[:, kk * width : (kk + 1) * width]
    corner(0)
    forward(*b_at)
    for k in range(1, first):
        corner(k)
    result = ref["d_two"][0, 0]
    for g in range(len(groups)):
        result = result + crossed(chunks, g, 2)
    arrive(*b_at)
    for q in range(cols):
        span = slice(q * fringe, (q + 1) * fringe)
        result = result - three(halves_of(ref["b"][q]), (ref["cl_h"][span], ref["cl_l"][span]))
    ref["o_two"][0, tiles + first] = result
    write(ref["o_two"].at[0, tiles:], ref["out_two"].at[0, tiles:])

    for go, wait in ends:
        if go is None:
            wait()
        else:
            pl.when(go)(wait)
    for copy in writes:
        copy.wait()


def leave(one, two, out_one, out_two, held_one, held_two, sems):
    pieces = [(one, held_one, out_one, k) for k in range(one.shape[0])] + [(two, held_two, out_two, 0)]

    def copy(source, target, k, index):
        return pltpu.make_async_copy(source.at[k], target.at[k], sems.at[index])

    ins = [copy(a, b, k, n) for n, (a, b, _, k) in enumerate(pieces)]
    outs = [copy(b, a, k, n + len(pieces)) for n, (_, b, a, k) in enumerate(pieces)]
    for each in ins:
        each.start()
    for taken, given in zip(ins, outs):
        taken.wait()
        given.start()
    for each in outs:
        each.wait()


def on_device_fused(
    ancestor,
    inverse_first,
    panel_first,
    structure_first,
    inverse_second,
    panel_second,
    structure_second,
):
    rows = lax.axis_size("row")
    cols = lax.axis_size("col")
    height = TILE // rows
    width = TILE // cols
    tiles = ancestor.shape[0]
    first = inverse_first.shape[0]
    entries = structure_first.shape[0]
    chunks = first + 1
    wide = tiles * width
    row_slots = tiles * height // GRAIN * CAP
    low_slots = first * height // GRAIN * CAP
    col_slots = wide // GRAIN * CAP
    row_pad = -(-row_slots // 128) * 128
    edge = first * height
    fringe = first * width
    parts = min(3, tiles)
    counts = [tiles // parts + (i < tiles % parts) for i in range(parts)]
    if counts[-1] > 1:
        counts[0] += 1
        counts[-1] -= 1
    groups = [(sum(counts[:i]), sum(counts[: i + 1])) for i in range(parts)]
    widest = max(stop - start for start, stop in groups) * width
    stages = chunks * parts
    dma = pltpu.SemaphoreType.DMA
    scratch = {
        "a": pltpu.VMEM((tiles, tiles, height, width), F32),
        "d_one": pltpu.VMEM((first, first, height, width), F32),
        "d_two": pltpu.VMEM((1, 1, height, width), F32),
        "l_one": pltpu.VMEM((entries,), jnp.int32),
        "l_two": pltpu.VMEM((entries,), jnp.int32),
        "o_one": pltpu.VMEM((first, tiles + first, height, width), F32),
        "o_two": pltpu.VMEM((1, tiles + first + 1, height, width), F32),
        "own": pltpu.VMEM((chunks, entries // rows, width), F32),
        "pall": pltpu.VMEM((chunks, entries, width), F32),
        "ph": pltpu.VMEM((entries, chunks * width), BF16),
        "pl": pltpu.VMEM((entries, chunks * width), BF16),
        "kept_h": pltpu.VMEM((2, row_pad, wide), BF16),
        "kept_l": pltpu.VMEM((2, row_pad, wide), BF16),
        "v_one": pltpu.VMEM((first, cols, row_slots, width), F32),
        "v_two": pltpu.VMEM((cols, row_slots + low_slots, width), F32),
        "turned": pltpu.VMEM((chunks, 8 * width, row_pad), BF16),
        "under": pltpu.VMEM((8 * width, edge), BF16),
        "y_h": pltpu.VMEM((chunks * height, wide), BF16),
        "y_l": pltpu.VMEM((chunks * height, wide), BF16),
        "d_h": pltpu.VMEM((edge, fringe), BF16),
        "d_l": pltpu.VMEM((edge, fringe), BF16),
        "pick": pltpu.VMEM((2, col_slots, widest), BF16),
        "cl_h": pltpu.VMEM((cols * fringe, width), BF16),
        "cl_l": pltpu.VMEM((cols * fringe, width), BF16),
        "b": pltpu.VMEM((cols, height, fringe), F32),
        "l_sem": dma((5 + chunks,)),
        "w_sem": dma((stages + first + 1,)),
        "g_send": dma((chunks,)),
        "g_recv": dma((chunks, 4)),
        "v_send": dma((chunks,)),
        "v_recv": dma((chunks, cols)),
        "r_send": dma((stages,)),
        "r_recv": dma((stages, 4)),
        "s_send": dma((chunks + 1, parts)),
        "s_recv": dma((chunks + 1, parts, cols)),
        "b_send": dma,
        "b_recv": dma((cols,)),
    }
    for g, (start, stop) in enumerate(groups):
        count = (stop - start) * width // GRAIN * CAP // 2
        region = -(-count * cols // 128) * 128
        for n in range(chunks + 1):
            scratch[f"s{n}{g}"] = pltpu.VMEM((cols, count, 2 * height), F32)
        for name in ("h", "l"):
            scratch[f"c1{g}{name}"] = pltpu.VMEM((2 * region, fringe), BF16)
            scratch[f"c2{g}{name}"] = pltpu.VMEM((2 * region, width), BF16)
    for s, (k, g) in enumerate(order_of(first, parts)):
        size = (groups[g][1] - groups[g][0]) * width
        if s == stages - 1:
            size += fringe
        scratch[f"z{s}"] = pltpu.VMEM((8, height, size), F32)
        scratch[f"m{s}"] = pltpu.VMEM((4, height, size), F32)
        scratch[f"t{s}"] = pltpu.VMEM((4, height, size), F32)
        scratch[f"i{s}"] = pltpu.VMEM((2, height // 2, size), F32)
        scratch[f"f{s}"] = pltpu.VMEM((4, height // 2, size), F32)
    inputs = ["ancestor", "diag_one", "diag_two", "panel_one", "panel_two", "list_one", "list_two"]
    names = inputs + ["out_one", "out_two"] + list(scratch)
    hbm = pl.BlockSpec(memory_space=pl.ANY)
    dims = (rows, cols, height, width, tiles, first, entries, groups)
    shapes = (
        jax.ShapeDtypeStruct((first, tiles + first, height, width), F32),
        jax.ShapeDtypeStruct((1, tiles + first + 1, height, width), F32),
    )
    results = pl.pallas_call(
        functools.partial(fused, dims, names),
        out_shape=shapes,
        in_specs=[hbm] * len(inputs),
        out_specs=(hbm, hbm),
        scratch_shapes=list(scratch.values()),
        compiler_params=pltpu.CompilerParams(
            collective_id=0, has_side_effects=True, vmem_limit_bytes=60 * 1024 * 1024
        ),
    )(
        open_packed(ancestor, height, width),
        open_packed(inverse_first, height, width),
        open_packed(inverse_second, height, width),
        panel_first,
        panel_second,
        structure_first,
        structure_second,
    )
    return pl.pallas_call(
        leave,
        out_shape=shapes,
        in_specs=[hbm, hbm],
        out_specs=(hbm, hbm),
        scratch_shapes=[
            pltpu.VMEM(shapes[0].shape, F32),
            pltpu.VMEM(shapes[1].shape, F32),
            dma((2 * (first + 1),)),
        ],
        compiler_params=pltpu.CompilerParams(vmem_limit_bytes=60 * 1024 * 1024),
    )(*results)


def fits(rows, cols):
    return rows == 8 and rows == 2 * cols and TILE // cols % 128 == 0


def solution(mesh):
    body = on_device_fused if fits(mesh.shape["row"], mesh.shape["col"]) else on_device
    in_specs = (
        P(None, None, "row", "col"),
        P(None, None, "row", "col"),
        P("row", None, "col"),
        P(),
        P(None, None, "row", "col"),
        P("row", None, "col"),
        P(),
    )
    out_specs = (P(None, None, "row", "col"), P(None, None, "row", "col"))
    return jax.shard_map(
        body, mesh=mesh, in_specs=in_specs, out_specs=out_specs, check_vma=False
    )
```

```python
import functools

import jax
import jax.numpy as jnp
from jax import lax
from jax.experimental import pallas as pl
from jax.experimental.pallas import tpu as pltpu
from jax.sharding import PartitionSpec as P

TILE = 512
GRAIN = 16
CAP = 6


def open_packed(packed, row_height, col_width):
    return packed.reshape(packed.shape[0], packed.shape[1], row_height, col_width)


def close_packed(tiles):
    depth = tiles.shape[2] * tiles.shape[3] // 128
    return tiles.reshape(tiles.shape[0], tiles.shape[1], depth, 128)


def product(left, right, left_dim=1):
    return lax.dot_general(
        left,
        right,
        (((left_dim,), (0,)), ((), ())),
        precision=lax.Precision.HIGH,
        preferred_element_type=jnp.float32,
    )


def entry_ranks(structure):
    group = structure // GRAIN
    order = jnp.arange(structure.shape[0], dtype=jnp.int32)
    same = (group[:, None] == group[None, :]) & (order[None, :] < order[:, None])
    return jnp.sum(same.astype(jnp.int32), axis=1)


def slots_within(structure, ranks, height):
    owner = structure % TILE // height
    group = structure // TILE * (height // GRAIN) + structure % height // GRAIN
    return owner, group * CAP + ranks


def one_hot(marks, count):
    return (jnp.arange(count, dtype=jnp.int32)[:, None] == marks[None, :]).astype(jnp.float32)


def local_rows(structure, marks, count, height):
    row = structure // TILE * height + structure % height
    match = jnp.arange(count, dtype=jnp.int32)[:, None] == marks[None, :]
    return jnp.max(jnp.where(match, row[None, :], -1), axis=1)


def on_device(
    ancestor,
    inverse_first,
    panel_first,
    structure_first,
    inverse_second,
    panel_second,
    structure_second,
):
    rows = lax.axis_size("row")
    cols = lax.axis_size("col")
    height = TILE // rows
    width = TILE // cols
    halves = width // height
    row_index = lax.axis_index("row")
    col_index = lax.axis_index("col")
    blocks = open_packed(ancestor, height, width)
    first_diag = open_packed(inverse_first, height, width)
    second_diag = open_packed(inverse_second, height, width)
    tiles = blocks.shape[0]
    first = first_diag.shape[0]
    second = second_diag.shape[0]
    every = first + second
    limit = tiles * TILE
    first_width = first * width

    panels = jnp.concatenate(
        [panel_first.reshape(-1, first_width), panel_second.reshape(-1, second * width)], axis=1
    )
    both = lax.all_gather(panels, "row", axis=0, tiled=True)
    whole_first = both[:, :first_width]
    whole_second = both[:, first_width:]

    above = structure_second < limit
    ranks_first = entry_ranks(structure_first)
    ranks_second = entry_ranks(structure_second)
    row_slots = tiles * height // GRAIN * CAP
    col_slots = tiles * width // GRAIN * CAP
    low_slots = first * TILE // GRAIN * CAP
    owner, slot = slots_within(structure_first, ranks_first, height)
    row_marks_first = jnp.where(owner == row_index, slot, -1)
    owner, slot = slots_within(structure_second, ranks_second, height)
    row_marks_second = jnp.where(above & (owner == row_index), slot, -1)
    owner, slot = slots_within(structure_first, ranks_first, width)
    all_marks_first = owner * col_slots + slot
    col_marks_first = jnp.where(owner == col_index, slot, -1)
    owner, slot = slots_within(structure_second, ranks_second, width)
    all_marks_second = jnp.where(above, owner * col_slots + slot, -1)
    col_marks_second = jnp.where(above & (owner == col_index), slot, -1)
    below = structure_second - limit
    low_marks = jnp.where(above, -1, below // GRAIN * CAP + ranks_second)
    low_match = jnp.arange(low_slots, dtype=jnp.int32)[:, None] == low_marks[None, :]
    low_rows = jnp.max(jnp.where(low_match, below[None, :], -1), axis=1)

    take_first = one_hot(row_marks_first, row_slots)
    take_second = one_hot(
        jnp.where(above, row_marks_second, row_slots + low_marks), row_slots + low_slots
    )
    part_first = product(take_first, whole_first)
    part_second = product(take_second, whole_second)
    part_first = part_first.reshape(row_slots, first, halves, height).transpose(0, 2, 1, 3)
    part_first = part_first.reshape(row_slots * first, width)
    part_second = part_second.reshape(row_slots + low_slots, second, halves, height)
    part_second = part_second.transpose(0, 2, 1, 3)
    part_second = part_second.reshape((row_slots + low_slots) * second, width)
    spread = lax.all_gather(jnp.concatenate([part_first, part_second], axis=0), "col", axis=0)
    cut = part_first.shape[0]
    got_first = spread[:, :cut].reshape(cols, row_slots, halves, first, height)
    got_second = spread[:, cut:].reshape(cols, row_slots + low_slots, halves, second, height)
    got_first = got_first.transpose(1, 0, 2, 3, 4).reshape(row_slots, rows, first * height)
    got_second = got_second.transpose(1, 0, 2, 3, 4).reshape(-1, rows, second * height)
    upper_second = got_second[:row_slots]
    low_second = got_second[row_slots:].reshape(low_slots, second * TILE)

    flat = blocks.transpose(0, 2, 1, 3).reshape(tiles * height, tiles * width)
    kept_rows = jnp.concatenate(
        [
            local_rows(structure_first, row_marks_first, row_slots, height),
            local_rows(structure_second, row_marks_second, row_slots, height),
        ]
    )
    take_kept = (
        kept_rows[:, None] == jnp.arange(tiles * height, dtype=jnp.int32)[None, :]
    ).astype(jnp.float32)
    kept = product(take_kept, flat)

    place = jnp.arange(first * TILE, dtype=jnp.int32)
    place_row = place // (first * height)
    place_tile = place // height % first
    named = place_tile * TILE + place_row * height + place % height
    meet_low = (named[:, None] == low_rows[None, :]).astype(jnp.float32)
    first_at_low = product(got_first.reshape(row_slots, first * TILE), meet_low)
    folded = product(first_at_low, low_second).reshape(row_slots, rows, second * height)
    left = jnp.concatenate(
        [
            jnp.concatenate([got_first, -folded], axis=2),
            jnp.concatenate(
                [jnp.zeros((row_slots, rows, first * height), jnp.float32), upper_second], axis=2
            ),
        ],
        axis=0,
    )
    partial = product(left.reshape(2 * row_slots, every * TILE), kept, 0)
    partial = partial.reshape(rows, every * height, tiles * width)

    own_low = jnp.arange(first * height, dtype=jnp.int32)
    own_low = own_low // height * TILE + row_index * height + own_low % height
    own_meet = (own_low[:, None] == low_rows[None, :]).astype(jnp.float32)
    own_second = product(own_meet, low_second)
    flat_diag = first_diag.transpose(0, 2, 1, 3).reshape(first * height, first_width)
    low_partial = product(own_second, flat_diag, 0)
    low_partial = low_partial.reshape(rows, second * height, first_width)

    slabs = [low_partial[:, :, k * width : (k + 1) * width] for k in range(first)]
    slabs.append(jnp.zeros((rows, (every - first * second) * height, width), jnp.float32))
    joined = jnp.concatenate([partial, jnp.concatenate(slabs, axis=1)], axis=2)
    summed = lax.psum_scatter(joined, "row", scatter_dimension=0, tiled=False)
    image = summed[:, : tiles * width]
    step = second * height
    low_image = jnp.concatenate(
        [summed[k * step : (k + 1) * step, tiles * width :] for k in range(first)], axis=1
    )

    edge = first * height
    column_ids = jnp.arange(tiles * width, dtype=jnp.int32)
    col_rows_first = local_rows(structure_first, col_marks_first, col_slots, width)
    col_rows_second = local_rows(structure_second, col_marks_second, col_slots, width)
    pick_first = (column_ids[:, None] == col_rows_first[None, :]).astype(jnp.float32)
    pick_second = (column_ids[:, None] == col_rows_second[None, :]).astype(jnp.float32)
    picked = jnp.concatenate([product(image, pick_first), product(image[edge:], pick_second)], axis=0)
    met = lax.all_gather(picked, "col", axis=0)
    met = met.transpose(1, 0, 2).reshape(-1, cols * col_slots)
    dense_first = product(one_hot(all_marks_first, cols * col_slots), whole_first)
    dense_second = product(one_hot(all_marks_second, cols * col_slots), whole_second)
    corner = product(met[: every * height], dense_first)
    low_block = low_image - corner[edge:]
    low_all = lax.all_gather(low_block, "col", axis=0)
    low_all = low_all.transpose(1, 0, 2).reshape(second * height, first * TILE)
    spot = jnp.arange(first * TILE, dtype=jnp.int32)
    spot = spot // width % first * TILE + spot // first_width * width + spot % width
    below_marks = jnp.where(above, -1, below)
    dense_low = product(
        (spot[:, None] == below_marks[None, :]).astype(jnp.float32), whole_second
    )
    final = product(met[every * height :], dense_second) + product(low_all, dense_low)

    def tiled(matrix, up, across):
        return matrix.reshape(up, height, across, width).transpose(0, 2, 1, 3)

    row_first = jnp.concatenate(
        [-tiled(image[:edge], first, tiles), first_diag + tiled(corner[:edge], first, first)], axis=1
    )
    row_second = jnp.concatenate(
        [
            -tiled(image[edge:], second, tiles),
            -tiled(low_block, second, first),
            second_diag + tiled(final, second, second),
        ],
        axis=1,
    )
    return (close_packed(row_first), close_packed(row_second))

F32 = jnp.float32
BF16 = jnp.bfloat16
MESH = pl.DeviceIdType.MESH


def over(value, size):
    return lax.shift_right_logical(value, jnp.int32(size.bit_length() - 1))


def within(value, size):
    return value & jnp.int32(size - 1)


def iota(shape, dim):
    return lax.broadcasted_iota(jnp.int32, shape, dim)


def ones_at(mask):
    return jnp.where(mask, 1.0, 0.0).astype(BF16)


def dd(left, right, left_dim=1, right_dim=0):
    return lax.dot_general(
        left, right, (((left_dim,), (right_dim,)), ((), ())), preferred_element_type=F32
    )


def halves_of(value):
    high = value.astype(BF16)
    return high, (value - high.astype(F32)).astype(BF16)


def three(left, right):
    return dd(left[0], right[0]) + dd(left[0], right[1]) + dd(left[1], right[0])


def grown(value, count):
    rest = count - value.shape[0]
    if not rest:
        return value
    return jnp.concatenate([value, jnp.zeros((rest, value.shape[1]), value.dtype)], axis=0)


def spots(hits, places):
    return jnp.max(jnp.where(hits, places, -1.0), axis=1, keepdims=True)


def order_of(first, parts):
    return [(k, g) for k in range(first + 1) for g in range(parts)]


def fused(dims, names, *refs):
    ref = dict(zip(names, refs))
    rows, cols, height, width, tiles, first, entries, groups = dims
    chunks = first + 1
    shard = entries // rows
    wide = tiles * width
    tall = tiles * height
    row_slots = tall // GRAIN * CAP
    low_slots = first * height // GRAIN * CAP
    tile_slots = width // GRAIN * CAP
    col_slots = tiles * tile_slots
    edge = first * height
    fringe = first * width
    row_pad = -(-row_slots // 128) * 128
    half = height // 2

    r = lax.axis_index("row")
    c = lax.axis_index("col")
    core = r % 2
    chip = r // 2
    chip_x = chip % 2
    chip_y = chip // 2
    by_x = r + 2 - 4 * chip_x
    by_y = r + 4 - 8 * chip_y
    by_both = r + 6 - 4 * chip_x - 8 * chip_y
    mate = r + 1 - 2 * core
    peers = {1: by_x, 2: by_y, 3: by_both}

    def chip_at(rel):
        x = 1 - chip_x if rel % 2 else chip_x
        y = 1 - chip_y if rel // 2 else chip_y
        return y * 2 + x

    ends = []

    def remote(source, target, send, recv, device, column=None):
        return pltpu.make_async_remote_copy(
            src_ref=source,
            dst_ref=target,
            send_sem=send,
            recv_sem=recv,
            device_id=(device, c if column is None else column),
            device_id_type=MESH,
        )

    def launch(copy):
        copy.start()
        return copy

    def sent(whole, sem, go=None):
        ends.append((go, lambda: remote(whole(), whole(), sem, sem, mate).wait_send()))

    barrier = pltpu.get_barrier_semaphore()
    for peer in (mate, by_x, by_y, by_both):
        pl.semaphore_signal(barrier, inc=1, device_id=(peer, c), device_id_type=MESH)
    for step in range(1, cols):
        other = (c + step) % cols
        pl.semaphore_signal(barrier, inc=1, device_id=(r, other), device_id_type=MESH)
    loads = {}

    def load(name, source, target):
        loads[name] = pltpu.make_async_copy(source, target, ref["l_sem"].at[len(loads)])
        loads[name].start()

    load("list_one", ref["list_one"], ref["l_one"])
    load("list_two", ref["list_two"], ref["l_two"])
    for k in range(chunks):
        source = ref["panel_one"].at[:, k] if k < first else ref["panel_two"].at[:, k - first]
        load(k, source, ref["own"].at[k])
    load("a", ref["ancestor"], ref["a"])
    load("d_one", ref["diag_one"], ref["d_one"])
    load("d_two", ref["diag_two"], ref["d_two"])

    def ranks(row):
        group = over(row, GRAIN)
        total = [jnp.zeros((1, 128), F32) for _ in range(entries // 128)]
        lanes = iota((128, 128), 1)
        order = iota((128, 128), 0)
        for b in range(entries // 128):
            one = group[:, b * 128 : (b + 1) * 128]
            column = jnp.broadcast_to(one, (128, 128)).T
            for t in range(b, entries // 128):
                hit = column == group[:, t * 128 : (t + 1) * 128]
                if t == b:
                    hit = hit & (order < lanes)
                total[t] = total[t] + jnp.sum(jnp.where(hit, 1.0, 0.0), axis=0, keepdims=True)
        return jnp.concatenate(total, axis=1).astype(jnp.int32)

    def owned(row, rank, size):
        owner = over(within(row, TILE), size)
        group = over(row, TILE) * (size // GRAIN) + over(within(row, size), GRAIN)
        place = over(row, TILE) * size + within(row, size)
        return owner, group * CAP + rank, place.astype(F32)

    loads["list_one"].wait()
    loads["list_two"].wait()
    row1 = ref["l_one"][...].reshape(1, entries)
    row2 = ref["l_two"][...].reshape(1, entries)
    rank1 = ranks(row1)
    rank2 = ranks(row2)
    above = row2 < tiles * TILE
    r_owner1, r_slot1, r_place1 = owned(row1, rank1, height)
    r_owner2, r_slot2, r_place2 = owned(row2, rank2, height)
    c_owner1, c_slot1, c_place1 = owned(row1, rank1, width)
    c_owner2, c_slot2, c_place2 = owned(row2, rank2, width)
    mark1 = jnp.where(r_owner1 == r, r_slot1, -1)
    mark2 = jnp.where(r_owner2 == r, r_slot2, -1)
    upper2 = jnp.where(above, mark2, -1)
    lower2 = jnp.where(above | (r_owner2 != r), -1, r_slot2 - row_slots)

    pl.semaphore_wait(barrier, 4 + cols - 1)
    pall = ref["pall"]

    def own_rows(device):
        return pl.ds(pl.multiple_of(device * shard, 8), shard)

    gather = {}
    for k in range(chunks):
        loads[k].wait()
        for rel, peer in (*peers.items(), (0, mate)):
            gather[k, rel] = launch(
                remote(
                    ref["own"].at[k],
                    pall.at[k, own_rows(r)],
                    ref["g_send"].at[k],
                    ref["g_recv"].at[k, rel],
                    peer,
                )
            )
        sent(lambda k=k: pall.at[k, pl.ds(0, 7 * shard)], ref["g_send"].at[k])
    for k in range(chunks):
        pall[k, own_rows(r), :] = ref["own"][k]

    def keep(at, marks, places):
        spot = spots(iota((row_pad, entries), 0) == marks, places)
        take = ones_at(spot == iota((row_pad, tall), 1).astype(F32))

        def step(j, carry):
            block = ref["a"][:, pl.ds(j, 1), :, :].reshape(tall, width)
            high, low = halves_of(block)
            span = pl.ds(pl.multiple_of(j * width, 128), width)
            ref["kept_h"][at, :, span] = dd(take, high).astype(BF16)
            ref["kept_l"][at, :, span] = dd(take, low).astype(BF16)
            return carry

        lax.fori_loop(0, tiles, step, 0)

    def spread(at, sends, recvs, whole, direct=False):
        for sign, reach in ((1, 3), (-1, 3), (1, 2), (-1, 2), (1, 1), (-1, 1)):
            there = c + sign * reach
            if reach < cols - 1 or direct:

                @pl.when((there >= 0) & (there < cols))
                def _(there=there):
                    remote(at(c), at(c), sends, recvs.at[c], r, there).start()

        if direct:
            sent(lambda: whole(cols - 1), sends)
        else:
            edge_of = (c == 0) | (c == cols - 1)
            sent(lambda: whole(2), sends, edge_of)
            sent(lambda: whole(4), sends, jnp.logical_not(edge_of))

    def forward(at, sends, recvs, whole, direct=False):
        if direct:
            return
        for sign in (1, -1):
            q = c - 2 * sign
            there = c + sign

            @pl.when((q >= 0) & (q < cols) & (there >= 0) & (there < cols))
            def _(q=q, there=there):
                copy = remote(at(q), at(q), sends, recvs.at[q], r, there)
                copy.wait_recv()
                copy.start()

    def arrive(at, sends, recvs, whole, direct=False):
        for reach in range(1, cols):
            for sign in (1, -1):
                q = c - reach * sign
                there = c + sign
                go = (q >= 0) & (q < cols)
                if reach == 2 and not direct:
                    go = go & ((there < 0) | (there >= cols))

                @pl.when(go)
                def _(q=q):
                    remote(at(q), at(q), sends, recvs.at[q], r, c).wait_recv()

    def v_at(k):
        buf = ref["v_one"].at[k] if k < first else ref["v_two"]
        return buf.at.__getitem__, ref["v_send"].at[k], ref["v_recv"].at[k], lambda n: buf.at[pl.ds(0, n)]

    one_rows = -(-row_slots // 16) * 16
    two_rows = -(-(row_slots + low_slots) // 16) * 16
    take1 = ones_at(iota((one_rows, entries), 0) == mark1)
    loads["a"].wait()
    keep(0, mark1, r_place1)
    for k in range(chunks):
        for rel in (1, 2, 3):
            gather[k, rel].wait_recv()
            part = pall.at[k, own_rows(peers[rel])]
            gather[k, 3 + rel] = launch(
                remote(part, part, ref["g_send"].at[k], ref["g_recv"].at[k, 0], mate)
            )
        four = pall.at[k, pl.ds(0, 4 * shard)]
        remote(four, four, ref["g_send"].at[k], ref["g_recv"].at[k, 0], mate).wait_recv()
        high, low = halves_of(pall[k])
        span = slice(k * width, (k + 1) * width)
        ref["ph"][:, span] = high
        ref["pl"][:, span] = low
        take = take1 if k < first else ones_at(iota((two_rows, entries), 0) == mark2)
        picked = dd(take, high) + dd(take, low)
        if k < first:
            ref["v_one"][k, pl.ds(c, 1)] = picked[None, :row_slots]
        else:
            ref["v_two"][pl.ds(c, 1)] = picked[None, : row_slots + low_slots]
        if k:
            forward(*v_at(k - 1))
        spread(*v_at(k))

    low_spot = spots(iota((128, entries), 0) == lower2, r_place2 - float(tall))
    spread_low = ones_at(low_spot == iota((128, edge), 1).astype(F32))
    loads["d_one"].wait()
    loads["d_two"].wait()
    for k in range(first):
        for kk in range(first):
            high, low = halves_of(ref["d_one"][k, kk])
            ref["d_h"][k * height : (k + 1) * height, kk * width : (kk + 1) * width] = high
            ref["d_l"][k * height : (k + 1) * height, kk * width : (kk + 1) * width] = low

    def picker(which, owner, slot, place, extra=None):
        mine = owner == c
        if extra is not None:
            mine = mine & extra
        spot = spots(iota((col_slots, entries), 0) == jnp.where(mine, slot, -1), place)
        for start, stop in groups:
            span = slice(start * tile_slots, stop * tile_slots)
            count = (stop - start) * width
            here = iota(((stop - start) * tile_slots, count), 1) + start * width
            ref["pick"][which, span, :count] = ones_at(spot[span] == here.astype(F32))

    def ready(k):
        arrive(*v_at(k))
        for rel in range(4):
            klass = chip_at(rel)
            if k < first:
                value = ref["v_one"][k, pl.ds(klass, 1)].reshape(row_slots, width)
            else:
                both = ref["v_two"][pl.ds(klass, 1)].reshape(row_slots + low_slots, width)
                value = both[:row_slots]
                under = halves_of(grown(both[row_slots:], 128).T)
                under = halves_of(dd(under[0], spread_low) + dd(under[1], spread_low))
                for n in range(2):
                    start = (4 * n + rel) * width
                    ref["under"][start : start + width, :] = under[n]
            turned = halves_of(grown(value, row_pad).T)
            for n in range(2):
                start = (4 * n + rel) * width
                ref["turned"][k, start : start + width, :] = turned[n]

    def stacked(left, high, low):
        count = left.shape[0] // 2
        both = dd(left, high)
        return both[:count] + both[count:] + dd(left[:count], low)

    stages = order_of(first, len(groups))
    names_of = {stage: s for s, stage in enumerate(stages)}
    live = {}

    def put(s, part, start, stop):
        for rel in range(4):
            for side in range(2):
                top = rel * width + side * height
                ref[f"z{s}"][side * 4 + rel, :, start:stop] = part[top : top + height]

    def begin(s):
        k, g = stages[s]
        start, stop = groups[g]
        span = slice(start * width, stop * width)
        count = (stop - start) * width
        at = 0 if k < first else 1
        part = stacked(ref["turned"][k], ref["kept_h"][at, :, span], ref["kept_l"][at, :, span])
        if k >= first:
            part = part - stacked(ref["under"][...], ref["y_h"][:edge, span], ref["y_l"][:edge, span])
        put(s, part, 0, count)
        if k >= first and g == len(groups) - 1:
            part = stacked(ref["under"][...], ref["d_h"][...], ref["d_l"][...])
            put(s, part, count, count + fringe)
        live[s, 0] = launch(
            remote(
                ref[f"z{s}"].at[pl.ds((1 - core) * 4, 4)],
                ref[f"m{s}"],
                ref["r_send"].at[s],
                ref["r_recv"].at[s, 0],
                mate,
            )
        )
        sent(lambda: ref[f"z{s}"].at[pl.ds(0, 7)], ref["r_send"].at[s])

    def strips(count, body):
        def step(i, carry):
            body(pl.multiple_of(i * 8, 8))
            return carry

        lax.fori_loop(0, count // 8, step, 0)

    def pass_on(s, index, source, target, peer):
        live[s, index] = launch(
            remote(source, target, ref["r_send"].at[s], ref["r_recv"].at[s, min(index, 3)], peer)
        )

    lower = pl.ds(0, half)
    upper = pl.ds(half, half)

    def push(s):
        live[s, 0].wait_recv()
        total = ref[f"t{s}"]
        got = ref[f"m{s}"]
        own = ref[f"z{s}"]
        count = total.shape[2]

        def pair(rel):
            def body(i):
                at = pl.ds(i, 8)
                mine = own[pl.ds(core * 4 + rel, 1), at, :].reshape(8, count)
                total[rel, at, :] = mine + got[rel, at, :]

            strips(height, body)

        pair(3)
        pass_on(s, 1, total.at[3, lower], ref[f"i{s}"].at[0], by_x)
        pass_on(s, 2, total.at[3, upper], ref[f"i{s}"].at[1], by_y)
        pair(1)
        pass_on(s, 3, total.at[1, lower], ref[f"f{s}"].at[0], by_x)
        pair(2)
        pass_on(s, 4, total.at[2, upper], ref[f"f{s}"].at[1], by_y)
        pair(0)

    summed = set()

    def middle(s):
        if s in summed:
            return
        summed.add(s)
        total = ref[f"t{s}"]
        live[s, 2].wait_recv()

        def body(i):
            at = pl.ds(pl.multiple_of(i + half, 8), 8)
            total[1, at, :] = total[1, at, :] + ref[f"i{s}"][1, pl.ds(i, 8), :]

        strips(half, body)
        pass_on(s, 5, total.at[1, upper], ref[f"f{s}"].at[2], by_x)
        live[s, 1].wait_recv()

        def body(i):
            at = pl.ds(i, 8)
            total[2, at, :] = total[2, at, :] + ref[f"i{s}"][0, at, :]

        strips(half, body)
        pass_on(s, 6, total.at[2, lower], ref[f"f{s}"].at[3], by_y)

    writes = []

    def write(source, target):
        copy = pltpu.make_async_copy(source, target, ref["w_sem"].at[len(writes)])
        copy.start()
        writes.append(copy)

    def counted(g):
        start, stop = groups[g]
        count = (stop - start) * tile_slots // 2
        return count, -(-count * cols // 128) * 128

    def s_at(n, g):
        buf = ref[f"s{n}{g}"]
        direct = n >= first and g == len(groups) - 1
        sems = ref["s_send"].at[n, g], ref["s_recv"].at[n, g]
        return buf.at.__getitem__, *sems, lambda k: buf.at[pl.ds(0, k)], direct

    def choose(n, g):
        start, stop = groups[g]
        top = start * tile_slots
        half_count = counted(g)[0]
        count = (stop - start) * width
        columns = slice(start * width, stop * width)
        which = n // chunks
        chunk = min(n, first) * height
        near = ref["pick"][which, top : top + half_count, :count]
        far = ref["pick"][which, top + half_count : top + 2 * half_count, :count]
        high = ref["y_h"][chunk : chunk + height, columns]
        low = ref["y_l"][chunk : chunk + height, columns]
        none = jnp.zeros_like(high)
        chosen = (
            dd(near, jnp.concatenate([high, none], axis=0), 1, 1)
            + dd(near, jnp.concatenate([low, none], axis=0), 1, 1)
            + dd(far, jnp.concatenate([none, high], axis=0), 1, 1)
            + dd(far, jnp.concatenate([none, low], axis=0), 1, 1)
        )
        ref[f"s{n}{g}"][pl.ds(c, 1)] = chosen[None]
        spread(*s_at(n, g))

    done = set()

    def finish(s):
        k, g = stages[s]
        start, stop = groups[g]
        fin = ref[f"f{s}"]
        remote(fin, fin, ref["r_send"].at[s], ref["r_recv"].at[s, 3], mate).wait_recv()
        out = ref[f"t{s}"]
        for base, one, two in ((0, 0, 3), (half, 1, 2)):

            def body(i, base=base, one=one, two=two):
                at = pl.ds(pl.multiple_of(i + base, 8), 8)
                out[0, at, :] = out[0, at, :] + (fin[one, pl.ds(i, 8), :] + fin[two, pl.ds(i, 8), :])

            strips(half, body)
        count = (stop - start) * width
        span = slice(start * width, stop * width)
        high, low = halves_of(out[0, :, :count])
        ref["y_h"][k * height : (k + 1) * height, span] = high
        ref["y_l"][k * height : (k + 1) * height, span] = low
        into, at, target = ("o_one", k, "out_one") if k < first else ("o_two", 0, "out_two")
        for j in range(start, stop):
            ref[into][at, j] = -out[0, :, (j - start) * width : (j + 1 - start) * width]
        write(ref[into].at[at, start:stop], ref[target].at[at, start:stop])
        done.add(s)
        choose(k, g)

    def order(at, owner, slot, g, keep_if):
        start, stop = groups[g]
        half_count, region = counted(g)
        inside = slot - start * tile_slots
        side = (inside >= half_count).astype(jnp.int32)
        mark = side * region + owner * half_count + inside - side * half_count
        mark = jnp.where((inside >= 0) & (inside < 2 * half_count) & keep_if, mark, -1)
        take = ones_at(iota((2 * region, entries), 0) == mark)
        span = slice(0, fringe) if at == 1 else slice(fringe, fringe + width)
        for part, name in (("ph", "h"), ("pl", "l")):
            ref[f"c{at}{g}{name}"][...] = dd(take, ref[part][:, span]).astype(BF16)

    def order_one(g):
        order(1, c_owner1, c_slot1, g, c_owner1 >= 0)

    def order_two(g):
        order(2, c_owner2, c_slot2, g, above)

    def order_low():
        place = (over(row2, TILE) - tiles) * width + within(row2, width)
        mark = jnp.where(above, -1, c_owner2 * fringe + place)
        take = ones_at(iota((cols * fringe, entries), 0) == mark)
        ref["cl_h"][...] = dd(take, ref["ph"][:, fringe:]).astype(BF16)
        ref["cl_l"][...] = dd(take, ref["pl"][:, fringe:]).astype(BF16)

    asides = {
        1: [lambda: keep(1, upper2, r_place2)],
        2: [
            lambda: forward(*v_at(first)),
            lambda: picker(0, c_owner1, c_slot1, c_place1),
            lambda: picker(1, c_owner2, c_slot2, c_place2, above),
        ],
    }
    for index, g in enumerate(range(len(groups))):
        asides.setdefault(3 + index, []).append(lambda g=g: order_one(g))
    pending = []
    begun = set()

    def settle(s, now):
        if s not in done:
            finish(s)
            if stages[s][0] < first:
                pending.append((now + 2, stages[s]))

    def relay(now):
        while pending and pending[0][0] <= now:
            forward(*s_at(*pending.pop(0)[1]))

    gap = 4
    count = len(stages)
    for step in range(count):
        if step >= gap:
            settle(step - gap, step)
        k, g = stages[step]
        if k not in begun:
            begun.add(k)
            ready(k)
        if k >= first:
            for s in range(first * len(groups)):
                middle(s)
            for other in range(first):
                settle(names_of[other, g], step)
        begin(step)
        if step >= 2:
            middle(step - 2)
        for work in asides.pop(step, []):
            work()
        push(step)
        relay(step)
    middle(count - 2)
    late = len(groups) - 1
    for g in range(len(groups)):
        if g == 1:
            middle(count - 1)
            relay(count + 2)
        finish(stages.index((first, g)))
        if g:
            forward(*s_at(first, g - 1))
    for g in range(len(groups)):
        choose(chunks, g)
    for g in range(late):
        order_two(g)
    forward(*s_at(chunks, 0))
    order_two(late)
    order_low()
    for g in range(1, late):
        forward(*s_at(chunks, g))

    def side_by_side(n, g):
        region = counted(g)[1]
        buf = ref[f"s{n}{g}"]
        return halves_of(grown(jnp.concatenate([buf[q] for q in range(cols)], axis=0), region).T)

    def ordered(at, g, side):
        region = counted(g)[1]
        span = slice(side * region, (side + 1) * region)
        return ref[f"c{at}{g}h"][span], ref[f"c{at}{g}l"][span]

    def crossed(n, g, at):
        arrive(*s_at(n, g))
        both = side_by_side(n, g)
        near = three(both, ordered(at, g, 0))[:height]
        return near + three(both, ordered(at, g, 1))[height:]

    def corner(k):
        total = jnp.zeros((height, fringe), F32)
        for g in range(len(groups)):
            total = total + crossed(k, g, 1)
        for kk in range(first):
            piece = total[:, kk * width : (kk + 1) * width]
            ref["o_one"][k, tiles + kk] = ref["d_one"][k, kk] + piece
        write(ref["o_one"].at[k, tiles:], ref["out_one"].at[k, tiles:])

    tail = ref[f"t{len(stages) - 1}"]
    cross = -tail[0, :, tail.shape[2] - fringe :]
    for g in range(len(groups)):
        cross = cross + crossed(first, g, 1)
    ref["b"][pl.ds(c, 1)] = cross[None]
    b_at = (
        ref["b"].at.__getitem__,
        ref["b_send"],
        ref["b_recv"],
        lambda n: ref["b"].at[pl.ds(0, n)],
    )
    spread(*b_at)
    for kk in range(first):
        ref["o_two"][0, tiles + kk] = cross[:, kk * width : (kk + 1) * width]
    corner(0)
    forward(*b_at)
    for k in range(1, first):
        corner(k)
    result = ref["d_two"][0, 0]
    for g in range(len(groups)):
        result = result + crossed(chunks, g, 2)
    arrive(*b_at)
    for q in range(cols):
        span = slice(q * fringe, (q + 1) * fringe)
        result = result - three(halves_of(ref["b"][q]), (ref["cl_h"][span], ref["cl_l"][span]))
    ref["o_two"][0, tiles + first] = result
    write(ref["o_two"].at[0, tiles:], ref["out_two"].at[0, tiles:])

    for go, wait in ends:
        if go is None:
            wait()
        else:
            pl.when(go)(wait)
    for copy in writes:
        copy.wait()


def leave(one, two, out_one, out_two, held_one, held_two, sems):
    pieces = [(one, held_one, out_one, k) for k in range(one.shape[0])] + [(two, held_two, out_two, 0)]

    def copy(source, target, k, index):
        return pltpu.make_async_copy(source.at[k], target.at[k], sems.at[index])

    ins = [copy(a, b, k, n) for n, (a, b, _, k) in enumerate(pieces)]
    outs = [copy(b, a, k, n + len(pieces)) for n, (_, b, a, k) in enumerate(pieces)]
    for each in ins:
        each.start()
    for taken, given in zip(ins, outs):
        taken.wait()
        given.start()
    for each in outs:
        each.wait()


def on_device_fused(
    ancestor,
    inverse_first,
    panel_first,
    structure_first,
    inverse_second,
    panel_second,
    structure_second,
):
    rows = lax.axis_size("row")
    cols = lax.axis_size("col")
    height = TILE // rows
    width = TILE // cols
    tiles = ancestor.shape[0]
    first = inverse_first.shape[0]
    entries = structure_first.shape[0]
    chunks = first + 1
    wide = tiles * width
    row_slots = tiles * height // GRAIN * CAP
    low_slots = first * height // GRAIN * CAP
    col_slots = wide // GRAIN * CAP
    row_pad = -(-row_slots // 128) * 128
    edge = first * height
    fringe = first * width
    parts = min(3, tiles)
    counts = [tiles // parts + (i < tiles % parts) for i in range(parts)]
    if counts[-1] > 1:
        counts[0] += 1
        counts[-1] -= 1
    groups = [(sum(counts[:i]), sum(counts[: i + 1])) for i in range(parts)]
    widest = max(stop - start for start, stop in groups) * width
    stages = chunks * parts
    dma = pltpu.SemaphoreType.DMA
    scratch = {
        "a": pltpu.VMEM((tiles, tiles, height, width), F32),
        "d_one": pltpu.VMEM((first, first, height, width), F32),
        "d_two": pltpu.VMEM((1, 1, height, width), F32),
        "l_one": pltpu.VMEM((entries,), jnp.int32),
        "l_two": pltpu.VMEM((entries,), jnp.int32),
        "o_one": pltpu.VMEM((first, tiles + first, height, width), F32),
        "o_two": pltpu.VMEM((1, tiles + first + 1, height, width), F32),
        "own": pltpu.VMEM((chunks, entries // rows, width), F32),
        "pall": pltpu.VMEM((chunks, entries, width), F32),
        "ph": pltpu.VMEM((entries, chunks * width), BF16),
        "pl": pltpu.VMEM((entries, chunks * width), BF16),
        "kept_h": pltpu.VMEM((2, row_pad, wide), BF16),
        "kept_l": pltpu.VMEM((2, row_pad, wide), BF16),
        "v_one": pltpu.VMEM((first, cols, row_slots, width), F32),
        "v_two": pltpu.VMEM((cols, row_slots + low_slots, width), F32),
        "turned": pltpu.VMEM((chunks, 8 * width, row_pad), BF16),
        "under": pltpu.VMEM((8 * width, edge), BF16),
        "y_h": pltpu.VMEM((chunks * height, wide), BF16),
        "y_l": pltpu.VMEM((chunks * height, wide), BF16),
        "d_h": pltpu.VMEM((edge, fringe), BF16),
        "d_l": pltpu.VMEM((edge, fringe), BF16),
        "pick": pltpu.VMEM((2, col_slots, widest), BF16),
        "cl_h": pltpu.VMEM((cols * fringe, width), BF16),
        "cl_l": pltpu.VMEM((cols * fringe, width), BF16),
        "b": pltpu.VMEM((cols, height, fringe), F32),
        "l_sem": dma((5 + chunks,)),
        "w_sem": dma((stages + first + 1,)),
        "g_send": dma((chunks,)),
        "g_recv": dma((chunks, 4)),
        "v_send": dma((chunks,)),
        "v_recv": dma((chunks, cols)),
        "r_send": dma((stages,)),
        "r_recv": dma((stages, 4)),
        "s_send": dma((chunks + 1, parts)),
        "s_recv": dma((chunks + 1, parts, cols)),
        "b_send": dma,
        "b_recv": dma((cols,)),
    }
    for g, (start, stop) in enumerate(groups):
        count = (stop - start) * width // GRAIN * CAP // 2
        region = -(-count * cols // 128) * 128
        for n in range(chunks + 1):
            scratch[f"s{n}{g}"] = pltpu.VMEM((cols, count, 2 * height), F32)
        for name in ("h", "l"):
            scratch[f"c1{g}{name}"] = pltpu.VMEM((2 * region, fringe), BF16)
            scratch[f"c2{g}{name}"] = pltpu.VMEM((2 * region, width), BF16)
    for s, (k, g) in enumerate(order_of(first, parts)):
        size = (groups[g][1] - groups[g][0]) * width
        if s == stages - 1:
            size += fringe
        scratch[f"z{s}"] = pltpu.VMEM((8, height, size), F32)
        scratch[f"m{s}"] = pltpu.VMEM((4, height, size), F32)
        scratch[f"t{s}"] = pltpu.VMEM((4, height, size), F32)
        scratch[f"i{s}"] = pltpu.VMEM((2, height // 2, size), F32)
        scratch[f"f{s}"] = pltpu.VMEM((4, height // 2, size), F32)
    inputs = ["ancestor", "diag_one", "diag_two", "panel_one", "panel_two", "list_one", "list_two"]
    names = inputs + ["out_one", "out_two"] + list(scratch)
    hbm = pl.BlockSpec(memory_space=pl.ANY)
    dims = (rows, cols, height, width, tiles, first, entries, groups)
    shapes = (
        jax.ShapeDtypeStruct((first, tiles + first, height, width), F32),
        jax.ShapeDtypeStruct((1, tiles + first + 1, height, width), F32),
    )
    results = pl.pallas_call(
        functools.partial(fused, dims, names),
        out_shape=shapes,
        in_specs=[hbm] * len(inputs),
        out_specs=(hbm, hbm),
        scratch_shapes=list(scratch.values()),
        compiler_params=pltpu.CompilerParams(
            collective_id=0, has_side_effects=True, vmem_limit_bytes=60 * 1024 * 1024
        ),
    )(
        open_packed(ancestor, height, width),
        open_packed(inverse_first, height, width),
        open_packed(inverse_second, height, width),
        panel_first,
        panel_second,
        structure_first,
        structure_second,
    )
    return pl.pallas_call(
        leave,
        out_shape=shapes,
        in_specs=[hbm, hbm],
        out_specs=(hbm, hbm),
        scratch_shapes=[
            pltpu.VMEM(shapes[0].shape, F32),
            pltpu.VMEM(shapes[1].shape, F32),
            dma((2 * (first + 1),)),
        ],
        compiler_params=pltpu.CompilerParams(vmem_limit_bytes=60 * 1024 * 1024),
    )(*results)


def fits(rows, cols):
    return rows == 8 and rows == 2 * cols and TILE // cols % 128 == 0


def solution(mesh):
    body = on_device_fused if fits(mesh.shape["row"], mesh.shape["col"]) else on_device
    in_specs = (
        P(None, None, "row", "col"),
        P(None, None, "row", "col"),
        P("row", None, "col"),
        P(),
        P(None, None, "row", "col"),
        P("row", None, "col"),
        P(),
    )
    out_specs = (P(None, None, "row", "col"), P(None, None, "row", "col"))
    return jax.shard_map(
        body, mesh=mesh, in_specs=in_specs, out_specs=out_specs, check_vma=False
    )
```
